8 devices in a mesh: data: 1 (over z), tp: 8 (over y, x, core).
Axes of the slice: x: 2, y: 2, z: 1, core: 2. Of those that a mesh axis runs over, the one named last changes fastest.
Arguments:
- attn_ctx: bfloat16 [512, 12288], P('data', 'tp')
- w_attn_out: bfloat16 [12288, 12288], P('tp')
- mlp_act: bfloat16 [512, 49152], P('data', 'tp')
- w_mlp_down: bfloat16 [49152, 12288], P('tp')
Outputs:
- output: bfloat16 [512, 12288], P('data')
All inputs are finite; a program needn't handle non-finite values.
Results may differ from the reference program's by a relative error of at most 0.0116369.
Values are sent between devices in bfloat16 or wider.
A program may use at most 1 GiB of HBM per device.

```python
import jax
import jax.numpy as jnp

TOKENS = 512
HIDDEN = 12288
FFN_DIM = 49152
ATTN_DIM = 12288


def setup_inputs(seed: int = 0, part: int = 0) -> dict:
    part_key = jax.random.fold_in(jax.random.key(seed), part)
    key_ctx, key_act = jax.random.split(part_key)
    key_wo, key_wd = jax.random.split(jax.random.key(seed + 1))
    w_scale = (FFN_DIM + ATTN_DIM) ** -0.5
    attn_ctx = jax.random.normal(key_ctx, (TOKENS, ATTN_DIM), jnp.float32)
    mlp_act = jax.random.normal(key_act, (TOKENS, FFN_DIM), jnp.float32)
    w_attn_out = jax.random.normal(key_wo, (ATTN_DIM, HIDDEN), jnp.float32) * w_scale
    w_mlp_down = jax.random.normal(key_wd, (FFN_DIM, HIDDEN), jnp.float32) * w_scale
    return {
        "attn_ctx": attn_ctx.astype(jnp.bfloat16),
        "w_attn_out": w_attn_out.astype(jnp.bfloat16),
        "mlp_act": mlp_act.astype(jnp.bfloat16),
        "w_mlp_down": w_mlp_down.astype(jnp.bfloat16),
    }


def reference(attn_ctx, w_attn_out, mlp_act, w_mlp_down):
    total = jnp.dot(attn_ctx, w_attn_out, preferred_element_type=jnp.float32)
    total = total + jnp.dot(mlp_act, w_mlp_down, preferred_element_type=jnp.float32)
    return total.astype(jnp.bfloat16)
```

```python
import functools

import jax
import jax.numpy as jnp
from jax import lax
from jax.experimental import pallas as pl
from jax.experimental.pallas import tpu as pltpu
from jax.sharding import PartitionSpec as P

MESH = pl.DeviceIdType.MESH
BF16 = jnp.bfloat16
F32 = jnp.float32

W = 512
D1, D2, D3, D4, D5 = 1, 3, 4, 5, 7
SLOTS = 4


def kernel(n_chunks, ctx_ref, wo_ref, act_ref, wd_ref, y_ref, x_v, w_v, recv0, recv1, recv2, send0, send1, send2, keep0, keep1, keep2, x_sem, w_sem, s_sem, r_sem):
    me = lax.axis_index("tp")
    core = lax.rem(me, 2)
    cx = lax.rem(me // 2, 2)
    cy = me // 4
    p_core = me + 1 - 2 * core
    p_x = me + 2 - 4 * cx
    p_y = me + 4 - 8 * cy
    ka = ctx_ref.shape[1]
    km = act_ref.shape[1]

    def half_rows(c):
        base = 256 * c
        h1 = [
            base + 64 * (1 - cx) + 32 * (1 - cy),
            base + 64 * (1 - cx) + 32 * cy,
            base + 64 * cx + 32 * (1 - cy),
            base + 64 * cx + 32 * cy,
        ]
        base = base + 128
        h2 = [
            base + 64 * (1 - cy) + 32 * (1 - cx),
            base + 64 * (1 - cy) + 32 * cx,
            base + 64 * cy + 32 * (1 - cx),
            base + 64 * cy + 32 * cx,
        ]
        return h1 + h2

    rows = half_rows(1 - core) + half_rows(core)
    base1 = 256 * core + 64 * cx
    base2 = 256 * core + 128 + 64 * cy
    own1 = base1 + 32 * cy
    own2 = base2 + 32 * cx

    def w_copies(c, slot):
        cols = pl.ds(pl.multiple_of(c * W, W), W)
        out = []
        for j in range(ka // 1536):
            out.append(pltpu.make_async_copy(wo_ref.at[pl.ds(j * 1536, 1536), cols], w_v.at[slot, pl.ds(j * 1536, 1536)], w_sem.at[slot, len(out)]))
        for j in range(km // 1536):
            out.append(pltpu.make_async_copy(wd_ref.at[pl.ds(j * 1536, 1536), cols], w_v.at[slot, pl.ds(ka + j * 1536, 1536)], w_sem.at[slot, len(out)]))
        return out

    for cp in w_copies(0, 0):
        cp.start()
    for b, r in enumerate(rows):
        r = pl.multiple_of(r, 32)
        pltpu.make_async_copy(ctx_ref.at[pl.ds(r, 32)], x_v.at[pl.ds(32 * b, 32), pl.ds(0, ka)], x_sem.at[0]).start()
        pltpu.make_async_copy(act_ref.at[pl.ds(r, 32)], x_v.at[pl.ds(32 * b, 32), pl.ds(ka, km)], x_sem.at[1]).start()

    barrier = pltpu.get_barrier_semaphore()
    for p in (p_core, p_x, p_y):
        pl.semaphore_signal(barrier, inc=1, device_id={"tp": p}, device_id_type=MESH)
    pl.semaphore_wait(barrier, 3)

    def remote(src, dst, k, c, to):
        return pltpu.make_async_remote_copy(
            src_ref=src, dst_ref=dst, send_sem=s_sem.at[k, lax.rem(c, SLOTS)], recv_sem=r_sem.at[k, c], device_id={"tp": to}, device_id_type=MESH
        )

    def y_at(r, n, c):
        return y_ref.at[pl.ds(pl.multiple_of(r, 32), n), pl.ds(pl.multiple_of(c * W, W), W)]

    def p0(c):
        return [remote(send0.at[lax.rem(c, 2)], recv0.at[c], 0, c, p_core)]

    def p1(c):
        s = lax.rem(c, SLOTS)
        return [remote(send1.at[s, 0], recv1.at[c, 0], 1, c, p_x), remote(send1.at[s, 1], recv1.at[c, 1], 2, c, p_y)]

    def p2(c):
        s = lax.rem(c, SLOTS)
        return [remote(send2.at[s, 0], recv2.at[c, 0], 3, c, p_y), remote(send2.at[s, 1], recv2.at[c, 1], 4, c, p_x)]

    def p3(c):
        return [remote(y_at(own1, 32, c), y_at(own1, 32, c), 5, c, p_y), remote(y_at(own2, 32, c), y_at(own2, 32, c), 6, c, p_x)]

    def p4(c):
        return [remote(y_at(base1, 64, c), y_at(base1, 64, c), 7, c, p_x), remote(y_at(base2, 64, c), y_at(base2, 64, c), 8, c, p_y)]

    def p5(c):
        half = 256 * core
        return [remote(y_at(half, 256, c), y_at(half, 256, c), 9, c, p_core)]

    def guard(cond, fn):
        if isinstance(cond, bool):
            if cond:
                fn()
        else:
            pl.when(cond)(fn)

    def drain(make, c):
        def fn():
            for d in make(c - SLOTS):
                d.wait_send()

        guard(c >= SLOTS, fn)

    def start(make, c):
        drain(make, c)
        for d in make(c):
            d.start()

    def stage0(c):
        for d in p0(c):
            d.wait_recv()
        k = lax.rem(c, SLOTS)
        drain(p1, c)
        for h in range(2):
            o = 128 * h
            send1[k, h] = (keep0[lax.rem(c, 2), o : o + 64] + recv0[c, o : o + 64].astype(F32)).astype(BF16)
            keep1[k, h] = keep0[lax.rem(c, 2), o + 64 : o + 128] + recv0[c, o + 64 : o + 128].astype(F32)
        for d in p1(c):
            d.start()

    def stage1(c):
        for d in p1(c):
            d.wait_recv()
        k = lax.rem(c, SLOTS)
        drain(p2, c)
        for h in range(2):
            send2[k, h] = (keep1[k, h, 0:32] + recv1[c, h, 0:32].astype(F32)).astype(BF16)
            keep2[k, h] = keep1[k, h, 32:64] + recv1[c, h, 32:64].astype(F32)
        for d in p2(c):
            d.start()

    def stage2(c):
        for d in p2(c):
            d.wait_recv()
        k = lax.rem(c, SLOTS)
        cols = pl.ds(pl.multiple_of(c * W, W), W)
        for h, r in enumerate((own1, own2)):
            y_ref[pl.ds(pl.multiple_of(r, 32), 32), cols] = (keep2[k, h] + recv2[c, h].astype(F32)).astype(BF16)
        start(p3, c)

    def stage3(c):
        for d in p3(c):
            d.wait_recv()
        start(p4, c)

    def stage4(c):
        for d in p4(c):
            d.wait_recv()
        start(p5, c)

    stages = ((D5, stage4), (D4, stage3), (D3, stage2), (D2, stage1), (D1, stage0))

    pltpu.make_async_copy(ctx_ref, x_v.at[:, pl.ds(0, ka)], x_sem.at[0]).wait()
    pltpu.make_async_copy(act_ref, x_v.at[:, pl.ds(ka, km)], x_sem.at[1]).wait()

    def step(i, carry):
        slot = lax.rem(i, 2)
        for cp in w_copies(i, slot):
            cp.wait()

        @pl.when(i + 1 < n_chunks)
        def _():
            for cp in w_copies(i + 1, 1 - slot):
                cp.start()

        @pl.when(i >= 2)
        def _():
            for d in p0(i - 2):
                d.wait_send()

        part = jnp.dot(x_v[...], w_v[slot], preferred_element_type=F32)
        send0[slot] = part[0:256].astype(BF16)
        keep0[slot] = part[256:512]
        for d in p0(i):
            d.start()
        for delay, fn in stages:
            pl.when(i >= delay)(functools.partial(fn, i - delay))
        return carry

    lax.fori_loop(0, n_chunks, step, 0)
    for i in range(n_chunks, n_chunks + D5):
        for delay, fn in stages:
            if 0 <= i - delay < n_chunks:
                fn(i - delay)
    for d in p0(n_chunks - 2) + p0(n_chunks - 1):
        d.wait_send()
    for c in range(n_chunks - SLOTS, n_chunks):
        for make in (p1, p2, p3, p4, p5):
            for d in make(c):
                d.wait_send()
    for c in range(n_chunks):
        for d in p5(c):
            d.wait_recv()


def solution(mesh):
    def device_step(ctx, w_out, act, w_down):
        rows, ka = ctx.shape
        km, cols = w_down.shape
        n = cols // W
        any_ = pl.BlockSpec(memory_space=pl.ANY)
        return pl.pallas_call(
            functools.partial(kernel, n),
            out_shape=jax.ShapeDtypeStruct((rows, cols), BF16),
            in_specs=[any_] * 4,
            out_specs=pl.BlockSpec(memory_space=pltpu.VMEM),
            scratch_shapes=[
                pltpu.VMEM((rows, ka + km), BF16),
                pltpu.VMEM((2, ka + km, W), BF16),
                pltpu.VMEM((n, 256, W), BF16),
                pltpu.VMEM((n, 2, 64, W), BF16),
                pltpu.VMEM((n, 2, 32, W), BF16),
                pltpu.VMEM((2, 256, W), BF16),
                pltpu.VMEM((SLOTS, 2, 64, W), BF16),
                pltpu.VMEM((SLOTS, 2, 32, W), BF16),
                pltpu.VMEM((2, 256, W), F32),
                pltpu.VMEM((SLOTS, 2, 64, W), F32),
                pltpu.VMEM((SLOTS, 2, 32, W), F32),
                pltpu.SemaphoreType.DMA((2,)),
                pltpu.SemaphoreType.DMA((2, (ka + km) // 1536)),
                pltpu.SemaphoreType.DMA((10, SLOTS)),
                pltpu.SemaphoreType.DMA((10, n)),
            ],
            compiler_params=pltpu.CompilerParams(collective_id=0, has_side_effects=True, vmem_limit_bytes=60 * 1024 * 1024),
            cost_estimate=pl.CostEstimate(flops=2 * rows * (ka + km) * cols, bytes_accessed=2 * (ka + km) * cols, transcendentals=0),
        )(ctx, w_out, act, w_down)

    return jax.shard_map(
        device_step,
        mesh=mesh,
        in_specs=(P("data", "tp"), P("tp", None), P("data", "tp"), P("tp", None)),
        out_specs=P("data", None),
        check_vma=False,
    )
```

```python
import functools

import jax
import jax.numpy as jnp
from jax import lax
from jax.experimental import pallas as pl
from jax.experimental.pallas import tpu as pltpu
from jax.sharding import PartitionSpec as P

MESH = pl.DeviceIdType.MESH
BF16 = jnp.bfloat16
F32 = jnp.float32

W = 512
D1, D2, D3, D4, D5 = 1, 3, 4, 5, 7
SLOTS = 4
VMEM_LIMIT = 44 * 1024 * 1024


def kernel(n_chunks, ctx_ref, wo_ref, act_ref, wd_ref, y_ref, x_v, w_v, recv0, recv1, recv2, send0, send1, send2, keep0, keep1, keep2, x_sem, w_sem, s_sem, r_sem):
    me = lax.axis_index("tp")
    core = lax.rem(me, 2)
    cx = lax.rem(me // 2, 2)
    cy = me // 4
    p_core = me + 1 - 2 * core
    p_x = me + 2 - 4 * cx
    p_y = me + 4 - 8 * cy
    ka = ctx_ref.shape[1]
    km = act_ref.shape[1]

    def half_rows(c):
        base = 256 * c
        h1 = [
            base + 64 * (1 - cx) + 32 * (1 - cy),
            base + 64 * (1 - cx) + 32 * cy,
            base + 64 * cx + 32 * (1 - cy),
            base + 64 * cx + 32 * cy,
        ]
        base = base + 128
        h2 = [
            base + 64 * (1 - cy) + 32 * (1 - cx),
            base + 64 * (1 - cy) + 32 * cx,
            base + 64 * cy + 32 * (1 - cx),
            base + 64 * cy + 32 * cx,
        ]
        return h1 + h2

    rows = half_rows(1 - core) + half_rows(core)
    base1 = 256 * core + 64 * cx
    base2 = 256 * core + 128 + 64 * cy
    own1 = base1 + 32 * cy
    own2 = base2 + 32 * cx

    def w_copies(c, slot):
        cols = pl.ds(pl.multiple_of(c * W, W), W)
        out = []
        for j in range(ka // 1536):
            out.append(pltpu.make_async_copy(wo_ref.at[pl.ds(j * 1536, 1536), cols], w_v.at[slot, pl.ds(j * 1536, 1536)], w_sem.at[slot, len(out)]))
        for j in range(km // 1536):
            out.append(pltpu.make_async_copy(wd_ref.at[pl.ds(j * 1536, 1536), cols], w_v.at[slot, pl.ds(ka + j * 1536, 1536)], w_sem.at[slot, len(out)]))
        return out

    for cp in w_copies(0, 0):
        cp.start()
    for b, r in enumerate(rows):
        r = pl.multiple_of(r, 32)
        pltpu.make_async_copy(ctx_ref.at[pl.ds(r, 32)], x_v.at[pl.ds(32 * b, 32), pl.ds(0, ka)], x_sem.at[0]).start()
        pltpu.make_async_copy(act_ref.at[pl.ds(r, 32)], x_v.at[pl.ds(32 * b, 32), pl.ds(ka, km)], x_sem.at[1]).start()

    barrier = pltpu.get_barrier_semaphore()
    for p in (p_core, p_x, p_y):
        pl.semaphore_signal(barrier, inc=1, device_id={"tp": p}, device_id_type=MESH)
    pl.semaphore_wait(barrier, 3)

    def remote(src, dst, k, c, to):
        return pltpu.make_async_remote_copy(
            src_ref=src, dst_ref=dst, send_sem=s_sem.at[k, lax.rem(c, SLOTS)], recv_sem=r_sem.at[k, c], device_id={"tp": to}, device_id_type=MESH
        )

    def y_at(r, n, c):
        return y_ref.at[pl.ds(pl.multiple_of(r, 32), n), pl.ds(pl.multiple_of(c * W, W), W)]

    def p0(c):
        return [remote(send0.at[lax.rem(c, 2)], recv0.at[c], 0, c, p_core)]

    def p1(c):
        s = lax.rem(c, SLOTS)
        return [remote(send1.at[s, 0], recv1.at[c, 0], 1, c, p_x), remote(send1.at[s, 1], recv1.at[c, 1], 2, c, p_y)]

    def p2(c):
        s = lax.rem(c, SLOTS)
        return [remote(send2.at[s, 0], recv2.at[c, 0], 3, c, p_y), remote(send2.at[s, 1], recv2.at[c, 1], 4, c, p_x)]

    def p3(c):
        return [remote(y_at(own1, 32, c), y_at(own1, 32, c), 5, c, p_y), remote(y_at(own2, 32, c), y_at(own2, 32, c), 6, c, p_x)]

    def p4(c):
        return [remote(y_at(base1, 64, c), y_at(base1, 64, c), 7, c, p_x), remote(y_at(base2, 64, c), y_at(base2, 64, c), 8, c, p_y)]

    def p5(c):
        half = 256 * core
        return [remote(y_at(half, 256, c), y_at(half, 256, c), 9, c, p_core)]

    def guard(cond, fn):
        if isinstance(cond, bool):
            if cond:
                fn()
        else:
            pl.when(cond)(fn)

    def drain(make, c):
        def fn():
            for d in make(c - SLOTS):
                d.wait_send()

        guard(c >= SLOTS, fn)

    def start(make, c):
        drain(make, c)
        for d in make(c):
            d.start()

    def stage0(c):
        for d in p0(c):
            d.wait_recv()
        k = lax.rem(c, SLOTS)
        drain(p1, c)
        for h in range(2):
            o = 128 * h
            send1[k, h] = (keep0[lax.rem(c, 2), o : o + 64] + recv0[c, o : o + 64].astype(F32)).astype(BF16)
            keep1[k, h] = keep0[lax.rem(c, 2), o + 64 : o + 128] + recv0[c, o + 64 : o + 128].astype(F32)
        for d in p1(c):
            d.start()

    def stage1(c):
        for d in p1(c):
            d.wait_recv()
        k = lax.rem(c, SLOTS)
        drain(p2, c)
        for h in range(2):
            send2[k, h] = (keep1[k, h, 0:32] + recv1[c, h, 0:32].astype(F32)).astype(BF16)
            keep2[k, h] = keep1[k, h, 32:64] + recv1[c, h, 32:64].astype(F32)
        for d in p2(c):
            d.start()

    def stage2(c):
        for d in p2(c):
            d.wait_recv()
        k = lax.rem(c, SLOTS)
        cols = pl.ds(pl.multiple_of(c * W, W), W)
        for h, r in enumerate((own1, own2)):
            y_ref[pl.ds(pl.multiple_of(r, 32), 32), cols] = (keep2[k, h] + recv2[c, h].astype(F32)).astype(BF16)
        start(p3, c)

    def stage3(c):
        for d in p3(c):
            d.wait_recv()
        start(p4, c)

    def stage4(c):
        for d in p4(c):
            d.wait_recv()
        start(p5, c)

    stages = ((D5, stage4), (D4, stage3), (D3, stage2), (D2, stage1), (D1, stage0))

    pltpu.make_async_copy(ctx_ref, x_v.at[:, pl.ds(0, ka)], x_sem.at[0]).wait()
    pltpu.make_async_copy(act_ref, x_v.at[:, pl.ds(ka, km)], x_sem.at[1]).wait()

    def step(i, carry):
        slot = lax.rem(i, 2)
        for cp in w_copies(i, slot):
            cp.wait()

        @pl.when(i + 1 < n_chunks)
        def _():
            for cp in w_copies(i + 1, 1 - slot):
                cp.start()

        @pl.when(i >= 2)
        def _():
            for d in p0(i - 2):
                d.wait_send()

        part = jnp.dot(x_v[...], w_v[slot], preferred_element_type=F32)
        send0[slot] = part[0:256].astype(BF16)
        keep0[slot] = part[256:512]
        for d in p0(i):
            d.start()
        for delay, fn in stages:
            pl.when(i >= delay)(functools.partial(fn, i - delay))
        return carry

    lax.fori_loop(0, n_chunks, step, 0)
    for i in range(n_chunks, n_chunks + D5):
        for delay, fn in stages:
            if 0 <= i - delay < n_chunks:
                fn(i - delay)
    for d in p0(n_chunks - 2) + p0(n_chunks - 1):
        d.wait_send()
    for c in range(n_chunks - SLOTS, n_chunks):
        for make in (p1, p2, p3, p4, p5):
            for d in make(c):
                d.wait_send()
    for c in range(n_chunks):
        for d in p5(c):
            d.wait_recv()


STORES = 8


def store(y_ref, o_ref, sem):
    n = y_ref.shape[0] // STORES
    copies = [pltpu.make_async_copy(y_ref.at[pl.ds(j * n, n)], o_ref.at[pl.ds(j * n, n)], sem.at[j]) for j in range(STORES)]
    for cp in copies:
        cp.start()
    for cp in copies:
        cp.wait()


def solution(mesh):
    def device_step(ctx, w_out, act, w_down):
        rows, ka = ctx.shape
        km, cols = w_down.shape
        n = cols // W
        any_ = pl.BlockSpec(memory_space=pl.ANY)
        y = pl.pallas_call(
            functools.partial(kernel, n),
            out_shape=pltpu.VMEM((rows, cols), BF16),
            in_specs=[any_] * 4,
            out_specs=pl.BlockSpec(memory_space=pltpu.VMEM),
            scratch_shapes=[
                pltpu.VMEM((rows, ka + km), BF16),
                pltpu.VMEM((2, ka + km, W), BF16),
                pltpu.VMEM((n, 256, W), BF16),
                pltpu.VMEM((n, 2, 64, W), BF16),
                pltpu.VMEM((n, 2, 32, W), BF16),
                pltpu.VMEM((2, 256, W), BF16),
                pltpu.VMEM((SLOTS, 2, 64, W), BF16),
                pltpu.VMEM((SLOTS, 2, 32, W), BF16),
                pltpu.VMEM((2, 256, W), F32),
                pltpu.VMEM((SLOTS, 2, 64, W), F32),
                pltpu.VMEM((SLOTS, 2, 32, W), F32),
                pltpu.SemaphoreType.DMA((2,)),
                pltpu.SemaphoreType.DMA((2, (ka + km) // 1536)),
                pltpu.SemaphoreType.DMA((10, SLOTS)),
                pltpu.SemaphoreType.DMA((10, n)),
            ],
            compiler_params=pltpu.CompilerParams(collective_id=0, has_side_effects=True, vmem_limit_bytes=VMEM_LIMIT),
            cost_estimate=pl.CostEstimate(flops=2 * rows * (ka + km) * cols, bytes_accessed=2 * (ka + km) * cols, transcendentals=0),
        )(ctx, w_out, act, w_down)
        return pl.pallas_call(
            store,
            out_shape=jax.ShapeDtypeStruct((rows, cols), BF16),
            in_specs=[pl.BlockSpec(memory_space=pltpu.VMEM)],
            out_specs=pl.BlockSpec(memory_space=pl.ANY),
            scratch_shapes=[pltpu.SemaphoreType.DMA((STORES,))],
            compiler_params=pltpu.CompilerParams(vmem_limit_bytes=1024 * 1024),
            cost_estimate=pl.CostEstimate(flops=0, bytes_accessed=2 * rows * cols, transcendentals=0),
        )(y)

    return jax.shard_map(
        device_step,
        mesh=mesh,
        in_specs=(P("data", "tp"), P("tp", None), P("data", "tp"), P("tp", None)),
        out_specs=P("data", None),
        check_vma=False,
    )
```

```python
import functools

import jax
import jax.numpy as jnp
from jax import lax
from jax.experimental import pallas as pl
from jax.experimental.pallas import tpu as pltpu
from jax.sharding import PartitionSpec as P

MESH = pl.DeviceIdType.MESH
BF16 = jnp.bfloat16
F32 = jnp.float32

W = 512
PARTS = 1
LAG = (1, 3, 5, 6, 8)
HEAD = 1
SLOTS = 4
STORES = 8
VMEM_LIMIT = 44 * 1024 * 1024
DRAIN = ((4, 8), (2, 5), (0, 1), (1, 3), (4, 7), (3, 6), (2, 4), (1, 2), (3, 5), (1, 1), (2, 3), (4, 6), (3, 4), (2, 2), (4, 5), (2, 1), (3, 3), (4, 4), (3, 2), (3, 1), (4, 3), (4, 2), (4, 1))


def kernel(n_chunks, ctx_ref, wo_ref, act_ref, wd_ref, y_ref, x_v, w_v, recv0, recv1, recv2, send0, send1, send2, keep0, keep1, keep2, x_sem, w_sem, s_sem, r_sem):
    me = lax.axis_index("tp")
    core = lax.rem(me, 2)
    cx = lax.rem(me // 2, 2)
    cy = me // 4
    p_core = me + 1 - 2 * core
    p_x = me + 2 - 4 * cx
    p_y = me + 4 - 8 * cy
    ka = ctx_ref.shape[1]
    km = act_ref.shape[1]

    def half_rows(c):
        base = 256 * c
        h1 = [
            base + 64 * (1 - cx) + 32 * (1 - cy),
            base + 64 * (1 - cx) + 32 * cy,
            base + 64 * cx + 32 * (1 - cy),
            base + 64 * cx + 32 * cy,
        ]
        base = base + 128
        h2 = [
            base + 64 * (1 - cy) + 32 * (1 - cx),
            base + 64 * (1 - cy) + 32 * cx,
            base + 64 * cy + 32 * (1 - cx),
            base + 64 * cy + 32 * cx,
        ]
        return h1 + h2

    rows = half_rows(1 - core) + half_rows(core)
    base1 = 256 * core + 64 * cx
    base2 = 256 * core + 128 + 64 * cy
    own1 = base1 + 32 * cy
    own2 = base2 + 32 * cx

    def w_copies(c, slot):
        cols = pl.ds(pl.multiple_of(c * W, W), W)
        out = []
        for j in range(ka // 1536):
            out.append(pltpu.make_async_copy(wo_ref.at[pl.ds(j * 1536, 1536), cols], w_v.at[slot, pl.ds(j * 1536, 1536)], w_sem.at[slot, len(out)]))
        for j in range(km // 1536):
            out.append(pltpu.make_async_copy(wd_ref.at[pl.ds(j * 1536, 1536), cols], w_v.at[slot, pl.ds(ka + j * 1536, 1536)], w_sem.at[slot, len(out)]))
        return out

    def x_copies(j):
        out = []
        for b, r in enumerate(rows):
            r = pl.multiple_of(r, 32)
            src = ctx_ref.at[pl.ds(r, 32), pl.ds(j * 1536, 1536)] if j * 1536 < ka else act_ref.at[pl.ds(r, 32), pl.ds(j * 1536 - ka, 1536)]
            out.append(pltpu.make_async_copy(src, x_v.at[pl.ds(32 * b, 32), pl.ds(j * 1536, 1536)], x_sem.at[j]))
        return out

    barrier = pltpu.get_barrier_semaphore()
    for p in (p_core, p_x, p_y):
        pl.semaphore_signal(barrier, inc=1, device_id={"tp": p}, device_id_type=MESH)
    n_slices = (ka + km) // 1536
    first = w_copies(0, 0)
    for j in range(n_slices):
        first[j].start()
        for cp in x_copies(j):
            cp.start()

    def remote(src, dst, k, c, to):
        return pltpu.make_async_remote_copy(
            src_ref=src, dst_ref=dst, send_sem=s_sem.at[k, lax.rem(c, SLOTS)], recv_sem=r_sem.at[k, c], device_id={"tp": to}, device_id_type=MESH
        )

    def y_at(r, n, c):
        return y_ref.at[pl.ds(pl.multiple_of(r, 32), n), pl.ds(pl.multiple_of(c * W, W), W)]

    def p0(c):
        return [remote(send0.at[lax.rem(c, 2)], recv0.at[c], 0, c, p_core)]

    def p1(c):
        s = lax.rem(c, SLOTS)
        return [remote(send1.at[s, 0], recv1.at[c, 0], 1, c, p_x), remote(send1.at[s, 1], recv1.at[c, 1], 2, c, p_y)]

    def p2(c):
        s = lax.rem(c, SLOTS)
        return [remote(send2.at[s, 0], recv2.at[c, 0], 3, c, p_y), remote(send2.at[s, 1], recv2.at[c, 1], 4, c, p_x)]

    def p3(c):
        return [remote(y_at(own1, 32, c), y_at(own1, 32, c), 5, c, p_y), remote(y_at(own2, 32, c), y_at(own2, 32, c), 6, c, p_x)]

    def p4(c):
        return [remote(y_at(base1, 64, c), y_at(base1, 64, c), 7, c, p_x), remote(y_at(base2, 64, c), y_at(base2, 64, c), 8, c, p_y)]

    def p5(c):
        half = 256 * core
        return [remote(y_at(half, 256, c), y_at(half, 256, c), 9, c, p_core)]

    def guard(cond, fn):
        if isinstance(cond, bool):
            if cond:
                fn()
        else:
            pl.when(cond)(fn)

    def drain(make, c):
        def fn():
            for d in make(c - SLOTS):
                d.wait_send()

        guard(c >= SLOTS, fn)

    def start(make, c):
        drain(make, c)
        for d in make(c):
            d.start()

    def stage0(c):
        for d in p0(c):
            d.wait_recv()
        k = lax.rem(c, SLOTS)
        drain(p1, c)
        for h in range(2):
            o = 128 * h
            send1[k, h] = (keep0[lax.rem(c, 2), o : o + 64] + recv0[c, o : o + 64].astype(F32)).astype(BF16)
            keep1[k, h] = keep0[lax.rem(c, 2), o + 64 : o + 128] + recv0[c, o + 64 : o + 128].astype(F32)
        for d in p1(c):
            d.start()

    def stage1(c):
        for d in p1(c):
            d.wait_recv()
        k = lax.rem(c, SLOTS)
        drain(p2, c)
        for h in range(2):
            send2[k, h] = (keep1[k, h, 0:32] + recv1[c, h, 0:32].astype(F32)).astype(BF16)
            keep2[k, h] = keep1[k, h, 32:64] + recv1[c, h, 32:64].astype(F32)
        for d in p2(c):
            d.start()

    def stage2(c):
        for d in p2(c):
            d.wait_recv()
        k = lax.rem(c, SLOTS)
        cols = pl.ds(pl.multiple_of(c * W, W), W)
        for h, r in enumerate((own1, own2)):
            y_ref[pl.ds(pl.multiple_of(r, 32), 32), cols] = (keep2[k, h] + recv2[c, h].astype(F32)).astype(BF16)
        start(p3, c)

    def stage3(c):
        for d in p3(c):
            d.wait_recv()
        start(p4, c)

    def stage4(c):
        for d in p4(c):
            d.wait_recv()
        start(p5, c)

    stages = (stage0, stage1, stage2, stage3, stage4)
    part_k = (ka + km) // PARTS

    def serve(i, q, static):
        for k in (4, 3, 2, 1, 0):
            back, rem = divmod(LAG[k] + PARTS - 1 - q, PARTS)
            if rem == 0:
                guard(i >= back, functools.partial(stages[k], i - back))

    def finish(i, slot, total):
        send0[slot] = total[0:256].astype(BF16)
        keep0[slot] = total[256:512]
        for d in p0(i):
            d.start()

    total = None
    for j in range(n_slices):
        first[j].wait()
        pltpu.make_async_copy(ctx_ref.at[:, pl.ds(0, 1536)], x_v.at[:, pl.ds(j * 1536, 1536)], x_sem.at[j]).wait()
        if j == 0:
            for cp in w_copies(1, 1):
                cp.start()
        piece = jnp.dot(x_v[:, j * 1536 : (j + 1) * 1536], w_v[0, j * 1536 : (j + 1) * 1536], preferred_element_type=F32)
        total = piece if total is None else total + piece
    pl.semaphore_wait(barrier, 3)
    finish(0, 0, total)

    def step(i, static):
        slot = i % 2 if static else lax.rem(i, 2)
        for cp in w_copies(i, slot):
            cp.wait()

        def ahead():
            for cp in w_copies(i + 1, 1 - slot):
                cp.start()

        guard(i + 1 < n_chunks, ahead)

        def sent():
            for d in p0(i - 2):
                d.wait_send()

        guard(i >= 2, sent)
        total = None
        for q in range(PARTS):
            piece = jnp.dot(x_v[:, q * part_k : (q + 1) * part_k], w_v[slot, q * part_k : (q + 1) * part_k], preferred_element_type=F32)
            total = piece if total is None else total + piece
            if q == PARTS - 1:
                finish(i, slot, total)
            serve(i, q, static)

    for i in range(1, HEAD):
        step(i, True)

    def looped(i, carry):
        step(i, False)
        return carry

    lax.fori_loop(HEAD, n_chunks, looped, 0)
    for k, back in DRAIN:
        stages[k](n_chunks - back)
    for d in p0(n_chunks - 2) + p0(n_chunks - 1):
        d.wait_send()
    for c in range(n_chunks - SLOTS, n_chunks):
        for make in (p1, p2, p3, p4, p5):
            for d in make(c):
                d.wait_send()
    for c in range(n_chunks):
        for d in p5(c):
            d.wait_recv()


def store(y_ref, o_ref, sem):
    n = y_ref.shape[0] // STORES
    copies = [pltpu.make_async_copy(y_ref.at[pl.ds(j * n, n)], o_ref.at[pl.ds(j * n, n)], sem.at[j]) for j in range(STORES)]
    for cp in copies:
        cp.start()
    for cp in copies:
        cp.wait()


def solution(mesh):
    def device_step(ctx, w_out, act, w_down):
        rows, ka = ctx.shape
        km, cols = w_down.shape
        n = cols // W
        any_ = pl.BlockSpec(memory_space=pl.ANY)
        y = pl.pallas_call(
            functools.partial(kernel, n),
            out_shape=pltpu.VMEM((rows, cols), BF16),
            in_specs=[any_] * 4,
            out_specs=pl.BlockSpec(memory_space=pltpu.VMEM),
            scratch_shapes=[
                pltpu.VMEM((rows, ka + km), BF16),
                pltpu.VMEM((2, ka + km, W), BF16),
                pltpu.VMEM((n, 256, W), BF16),
                pltpu.VMEM((n, 2, 64, W), BF16),
                pltpu.VMEM((n, 2, 32, W), BF16),
                pltpu.VMEM((2, 256, W), BF16),
                pltpu.VMEM((SLOTS, 2, 64, W), BF16),
                pltpu.VMEM((SLOTS, 2, 32, W), BF16),
                pltpu.VMEM((2, 256, W), F32),
                pltpu.VMEM((SLOTS, 2, 64, W), F32),
                pltpu.VMEM((SLOTS, 2, 32, W), F32),
                pltpu.SemaphoreType.DMA(((ka + km) // 1536,)),
                pltpu.SemaphoreType.DMA((2, (ka + km) // 1536)),
                pltpu.SemaphoreType.DMA((10, SLOTS)),
                pltpu.SemaphoreType.DMA((10, n)),
            ],
            compiler_params=pltpu.CompilerParams(collective_id=0, has_side_effects=True, vmem_limit_bytes=VMEM_LIMIT),
            cost_estimate=pl.CostEstimate(flops=2 * rows * (ka + km) * cols, bytes_accessed=2 * (ka + km) * cols, transcendentals=0),
        )(ctx, w_out, act, w_down)
        return pl.pallas_call(
            store,
            out_shape=jax.ShapeDtypeStruct((rows, cols), BF16),
            in_specs=[pl.BlockSpec(memory_space=pltpu.VMEM)],
            out_specs=pl.BlockSpec(memory_space=pl.ANY),
            scratch_shapes=[pltpu.SemaphoreType.DMA((STORES,))],
            compiler_params=pltpu.CompilerParams(vmem_limit_bytes=1024 * 1024),
            cost_estimate=pl.CostEstimate(flops=0, bytes_accessed=2 * rows * cols, transcendentals=0),
        )(y)

    return jax.shard_map(
        device_step,
        mesh=mesh,
        in_specs=(P("data", "tp"), P("tp", None), P("data", "tp"), P("tp", None)),
        out_specs=P("data", None),
        check_vma=False,
    )
```

```python
import functools

import jax
import jax.numpy as jnp
from jax import lax
from jax.experimental import pallas as pl
from jax.experimental.pallas import tpu as pltpu
from jax.sharding import PartitionSpec as P

MESH = pl.DeviceIdType.MESH
BF16 = jnp.bfloat16
F32 = jnp.float32

W = 512
K = 256
CUTS = (0, 5, 15, 26, 30)
LAG = ((1, 1), (3, 1), (4, 1), (5, 0), (6, 0))
HEAD = 6
UNROLL = 2
SLOTS = 4
STORES = 8
VMEM_LIMIT = 48 * 1024 * 1024
DRAIN = ((1, 3), (4, 6), (3, 5), (2, 4), (0, 1), (1, 2), (2, 3), (4, 5), (3, 4), (1, 1), (2, 2), (3, 3), (4, 4), (2, 1), (3, 2), (4, 3), (3, 1), (4, 2), (4, 1))


def kernel(n_chunks, ctx_ref, wo_ref, act_ref, wd_ref, y_ref, x_v, w_v, recv0, recv1, recv2, send0, send1, send2, keep0, keep1, keep2, x_sem, w_sem, s_sem, r_sem):
    me = lax.axis_index("tp")
    core = lax.rem(me, 2)
    cx = lax.rem(me // 2, 2)
    cy = me // 4
    p_core = me + 1 - 2 * core
    p_x = me + 2 - 4 * cx
    p_y = me + 4 - 8 * cy
    ka = ctx_ref.shape[1]
    km = act_ref.shape[1]

    def half_rows(c):
        base = 256 * c
        h1 = [
            base + 64 * (1 - cx) + 32 * (1 - cy),
            base + 64 * (1 - cx) + 32 * cy,
            base + 64 * cx + 32 * (1 - cy),
            base + 64 * cx + 32 * cy,
        ]
        base = base + 128
        h2 = [
            base + 64 * (1 - cy) + 32 * (1 - cx),
            base + 64 * (1 - cy) + 32 * cx,
            base + 64 * cy + 32 * (1 - cx),
            base + 64 * cy + 32 * cx,
        ]
        return h1 + h2

    rows = half_rows(1 - core) + half_rows(core)
    base1 = 256 * core + 64 * cx
    base2 = 256 * core + 128 + 64 * cy
    own1 = base1 + 32 * cy
    own2 = base2 + 32 * cx

    def w_copies(c, slot):
        cols = pl.ds(pl.multiple_of(c * W, W), W)
        out = []
        for j in range(ka // 1536):
            out.append(pltpu.make_async_copy(wo_ref.at[pl.ds(j * 1536, 1536), cols], w_v.at[slot, pl.ds(j * 1536, 1536)], w_sem.at[slot, len(out)]))
        for j in range(km // 1536):
            out.append(pltpu.make_async_copy(wd_ref.at[pl.ds(j * 1536, 1536), cols], w_v.at[slot, pl.ds(ka + j * 1536, 1536)], w_sem.at[slot, len(out)]))
        return out

    def x_copies(j):
        out = []
        for b, r in enumerate(rows):
            r = pl.multiple_of(r, 32)
            src = ctx_ref.at[pl.ds(r, 32), pl.ds(j * 1536, 1536)] if j * 1536 < ka else act_ref.at[pl.ds(r, 32), pl.ds(j * 1536 - ka, 1536)]
            out.append(pltpu.make_async_copy(src, x_v.at[pl.ds(32 * b, 32), pl.ds(j * 1536, 1536)], x_sem.at[j]))
        return out

    barrier = pltpu.get_barrier_semaphore()
    for p in (p_core, p_x, p_y):
        pl.semaphore_signal(barrier, inc=1, device_id={"tp": p}, device_id_type=MESH)
    n_slices = (ka + km) // 1536
    first = w_copies(0, 0)
    for j in range(n_slices):
        first[j].start()
        for cp in x_copies(j):
            cp.start()

    def remote(src, dst, k, c, to):
        return pltpu.make_async_remote_copy(
            src_ref=src, dst_ref=dst, send_sem=s_sem.at[k, lax.rem(c, SLOTS)], recv_sem=r_sem.at[k, c], device_id={"tp": to}, device_id_type=MESH
        )

    def y_at(r, n, c):
        return y_ref.at[pl.ds(pl.multiple_of(r, 32), n), pl.ds(pl.multiple_of(c * W, W), W)]

    def p0(c):
        return [remote(send0.at[lax.rem(c, 2)], recv0.at[c], 0, c, p_core)]

    def p1(c):
        s = lax.rem(c, SLOTS)
        return [remote(send1.at[s, 0], recv1.at[c, 0], 1, c, p_x), remote(send1.at[s, 1], recv1.at[c, 1], 2, c, p_y)]

    def p2(c):
        s = lax.rem(c, SLOTS)
        return [remote(send2.at[s, 0], recv2.at[c, 0], 3, c, p_y), remote(send2.at[s, 1], recv2.at[c, 1], 4, c, p_x)]

    def p3(c):
        return [remote(y_at(own1, 32, c), y_at(own1, 32, c), 5, c, p_y), remote(y_at(own2, 32, c), y_at(own2, 32, c), 6, c, p_x)]

    def p4(c):
        return [remote(y_at(base1, 64, c), y_at(base1, 64, c), 7, c, p_x), remote(y_at(base2, 64, c), y_at(base2, 64, c), 8, c, p_y)]

    def p5(c):
        half = 256 * core
        return [remote(y_at(half, 256, c), y_at(half, 256, c), 9, c, p_core)]

    def guard(cond, fn):
        if isinstance(cond, bool):
            if cond:
                fn()
        else:
            pl.when(cond)(fn)

    def drain(make, c):
        def fn():
            for d in make(c - SLOTS):
                d.wait_send()

        guard(c >= SLOTS, fn)

    def start(make, c):
        drain(make, c)
        for d in make(c):
            d.start()

    def stage0(c):
        for d in p0(c):
            d.wait_recv()
        k = lax.rem(c, SLOTS)
        drain(p1, c)
        for h in range(2):
            o = 128 * h
            send1[k, h] = (keep0[lax.rem(c, 2), o : o + 64] + recv0[c, o : o + 64].astype(F32)).astype(BF16)
            keep1[k, h] = keep0[lax.rem(c, 2), o + 64 : o + 128] + recv0[c, o + 64 : o + 128].astype(F32)
        for d in p1(c):
            d.start()

    def stage1(c):
        for d in p1(c):
            d.wait_recv()
        k = lax.rem(c, SLOTS)
        drain(p2, c)
        for h in range(2):
            send2[k, h] = (keep1[k, h, 0:32] + recv1[c, h, 0:32].astype(F32)).astype(BF16)
            keep2[k, h] = keep1[k, h, 32:64] + recv1[c, h, 32:64].astype(F32)
        for d in p2(c):
            d.start()

    def stage2(c):
        for d in p2(c):
            d.wait_recv()
        k = lax.rem(c, SLOTS)
        cols = pl.ds(pl.multiple_of(c * W, W), W)
        for h, r in enumerate((own1, own2)):
            y_ref[pl.ds(pl.multiple_of(r, 32), 32), cols] = (keep2[k, h] + recv2[c, h].astype(F32)).astype(BF16)
        start(p3, c)

    def stage3(c):
        for d in p3(c):
            d.wait_recv()
        start(p4, c)

    def stage4(c):
        for d in p4(c):
            d.wait_recv()
        start(p5, c)

    stages = (stage0, stage1, stage2, stage3, stage4)

    def serve(i, cut, static):
        for k in (4, 3, 2, 1, 0):
            back, at = LAG[k]
            if at == cut and (not static or i >= back):
                stages[k](i - back)

    def finish(c, slot, total):
        def sent():
            for d in p0(c - 2):
                d.wait_send()

        guard(c >= 2, sent)
        send0[slot] = total[0:256].astype(BF16)
        keep0[slot] = total[256:512]
        for d in p0(c):
            d.start()

    def ahead(i, slot):
        def fn():
            for cp in w_copies(i + 1, 1 - slot):
                cp.start()

        guard(i + 1 < n_chunks, fn)

    def here(i, slot):
        def fn():
            for cp in w_copies(i, slot):
                cp.wait()

        guard(i < n_chunks, fn)

    def chunk(i, slot, before, static):
        total = None
        for cut in range(4):
            k0, k1 = CUTS[cut] * K, CUTS[cut + 1] * K
            piece = jnp.dot(x_v[:, k0:k1], w_v[slot, k0:k1], preferred_element_type=F32)
            total = piece if total is None else piece + total
            if cut == 0:
                ahead(i, slot)
                if before is not None:
                    finish(i - 1, 1 - slot, before)
            if cut < 2:
                serve(i, cut, static)
            if cut == 2:
                here(i + 1, 1 - slot)
        return total

    pl.semaphore_wait(barrier, 3)
    total = None
    for j in range(n_slices):
        first[j].wait()
        pltpu.make_async_copy(ctx_ref.at[:, pl.ds(0, 1536)], x_v.at[:, pl.ds(j * 1536, 1536)], x_sem.at[j]).wait()
        if j == 0:
            ahead(0, 0)
        piece = jnp.dot(x_v[:, j * 1536 : (j + 1) * 1536], w_v[0, j * 1536 : (j + 1) * 1536], preferred_element_type=F32)
        total = piece if total is None else piece + total
        if j == n_slices - 2:
            here(1, 1)
    for i in range(1, HEAD):
        total = chunk(i, i % 2, total, True)
    finish(HEAD - 1, (HEAD - 1) % 2, total)

    def looped(j, carry):
        total = None
        for h in range(UNROLL):
            total = chunk(HEAD + UNROLL * j + h, h % 2, total, False)
        finish(HEAD + UNROLL * j + UNROLL - 1, 1, total)
        return carry

    lax.fori_loop(0, (n_chunks - HEAD) // UNROLL, looped, 0)
    for k, back in DRAIN:
        stages[k](n_chunks - back)
    for d in p0(n_chunks - 2) + p0(n_chunks - 1):
        d.wait_send()
    for c in range(n_chunks - SLOTS, n_chunks):
        for make in (p1, p2, p3, p4, p5):
            for d in make(c):
                d.wait_send()
    for c in range(n_chunks):
        for d in p5(c):
            d.wait_recv()


def store(y_ref, o_ref, sem):
    n = y_ref.shape[0] // STORES
    copies = [pltpu.make_async_copy(y_ref.at[pl.ds(j * n, n)], o_ref.at[pl.ds(j * n, n)], sem.at[j]) for j in range(STORES)]
    for cp in copies:
        cp.start()
    for cp in copies:
        cp.wait()


def solution(mesh):
    def device_step(ctx, w_out, act, w_down):
        rows, ka = ctx.shape
        km, cols = w_down.shape
        n = cols // W
        any_ = pl.BlockSpec(memory_space=pl.ANY)
        y = pl.pallas_call(
            functools.partial(kernel, n),
            out_shape=pltpu.VMEM((rows, cols), BF16),
            in_specs=[any_] * 4,
            out_specs=pl.BlockSpec(memory_space=pltpu.VMEM),
            scratch_shapes=[
                pltpu.VMEM((rows, ka + km), BF16),
                pltpu.VMEM((2, ka + km, W), BF16),
                pltpu.VMEM((n, 256, W), BF16),
                pltpu.VMEM((n, 2, 64, W), BF16),
                pltpu.VMEM((n, 2, 32, W), BF16),
                pltpu.VMEM((2, 256, W), BF16),
                pltpu.VMEM((SLOTS, 2, 64, W), BF16),
                pltpu.VMEM((SLOTS, 2, 32, W), BF16),
                pltpu.VMEM((2, 256, W), F32),
                pltpu.VMEM((SLOTS, 2, 64, W), F32),
                pltpu.VMEM((SLOTS, 2, 32, W), F32),
                pltpu.SemaphoreType.DMA(((ka + km) // 1536,)),
                pltpu.SemaphoreType.DMA((2, (ka + km) // 1536)),
                pltpu.SemaphoreType.DMA((10, SLOTS)),
                pltpu.SemaphoreType.DMA((10, n)),
            ],
            compiler_params=pltpu.CompilerParams(collective_id=0, has_side_effects=True, vmem_limit_bytes=VMEM_LIMIT),
            cost_estimate=pl.CostEstimate(flops=2 * rows * (ka + km) * cols, bytes_accessed=2 * (ka + km) * cols, transcendentals=0),
        )(ctx, w_out, act, w_down)
        return pl.pallas_call(
            store,
            out_shape=jax.ShapeDtypeStruct((rows, cols), BF16),
            in_specs=[pl.BlockSpec(memory_space=pltpu.VMEM)],
            out_specs=pl.BlockSpec(memory_space=pl.ANY),
            scratch_shapes=[pltpu.SemaphoreType.DMA((STORES,))],
            compiler_params=pltpu.CompilerParams(vmem_limit_bytes=1024 * 1024),
            cost_estimate=pl.CostEstimate(flops=0, bytes_accessed=2 * rows * cols, transcendentals=0),
        )(y)

    return jax.shard_map(
        device_step,
        mesh=mesh,
        in_specs=(P("data", "tp"), P("tp", None), P("data", "tp"), P("tp", None)),
        out_specs=P("data", None),
        check_vma=False,
    )
```

```python
import functools

import jax
import jax.numpy as jnp
from jax import lax
from jax.experimental import pallas as pl
from jax.experimental.pallas import tpu as pltpu
from jax.sharding import PartitionSpec as P

MESH = pl.DeviceIdType.MESH
BF16 = jnp.bfloat16
F32 = jnp.float32

W = 512
PARTS = 1
LAG = (1, 2, 3, 4, 5)
HEAD = 1
SLOTS = 4
DELAY = 3840
STORES = 8
VMEM_LIMIT = 44 * 1024 * 1024
DRAIN = ((4, 5), (3, 4), (0, 1), (2, 3), (1, 2), (4, 4), (1, 1), (3, 3), (2, 2), (2, 1), (4, 3), (3, 2), (3, 1), (4, 2), (4, 1))


def kernel(n_chunks, ctx_ref, wo_ref, act_ref, wd_ref, y_ref, x_v, w_v, recv0, recv1, recv2, send0, send1, send2, keep0, keep1, keep2, wait_v, x_sem, w_sem, s_sem, r_sem):
    me = lax.axis_index("tp")
    core = lax.rem(me, 2)
    cx = lax.rem(me // 2, 2)
    cy = me // 4
    p_core = me + 1 - 2 * core
    p_x = me + 2 - 4 * cx
    p_y = me + 4 - 8 * cy
    ka = ctx_ref.shape[1]
    km = act_ref.shape[1]

    def half_rows(c):
        base = 256 * c
        h1 = [
            base + 64 * (1 - cx) + 32 * (1 - cy),
            base + 64 * (1 - cx) + 32 * cy,
            base + 64 * cx + 32 * (1 - cy),
            base + 64 * cx + 32 * cy,
        ]
        base = base + 128
        h2 = [
            base + 64 * (1 - cy) + 32 * (1 - cx),
            base + 64 * (1 - cy) + 32 * cx,
            base + 64 * cy + 32 * (1 - cx),
            base + 64 * cy + 32 * cx,
        ]
        return h1 + h2

    rows = half_rows(1 - core) + half_rows(core)
    base1 = 256 * core + 64 * cx
    base2 = 256 * core + 128 + 64 * cy
    own1 = base1 + 32 * cy
    own2 = base2 + 32 * cx

    def w_copies(c, slot):
        cols = pl.ds(pl.multiple_of(c * W, W), W)
        out = []
        for j in range(ka // 1536):
            out.append(pltpu.make_async_copy(wo_ref.at[pl.ds(j * 1536, 1536), cols], w_v.at[slot, pl.ds(j * 1536, 1536)], w_sem.at[slot, len(out)]))
        for j in range(km // 1536):
            out.append(pltpu.make_async_copy(wd_ref.at[pl.ds(j * 1536, 1536), cols], w_v.at[slot, pl.ds(ka + j * 1536, 1536)], w_sem.at[slot, len(out)]))
        return out

    def x_copies(j):
        out = []
        for b, r in enumerate(rows):
            r = pl.multiple_of(r, 32)
            src = ctx_ref.at[pl.ds(r, 32), pl.ds(j * 1536, 1536)] if j * 1536 < ka else act_ref.at[pl.ds(r, 32), pl.ds(j * 1536 - ka, 1536)]
            out.append(pltpu.make_async_copy(src, x_v.at[pl.ds(32 * b, 32), pl.ds(j * 1536, 1536)], x_sem.at[j]))
        return out

    barrier = pltpu.get_barrier_semaphore()
    for p in (p_core, p_x, p_y):
        pl.semaphore_signal(barrier, inc=1, device_id={"tp": p}, device_id_type=MESH)
    n_slices = (ka + km) // 1536
    first = w_copies(0, 0)
    for j in range(n_slices):
        first[j].start()
        for cp in x_copies(j):
            cp.start()

    def remote(src, dst, k, c, to):
        return pltpu.make_async_remote_copy(
            src_ref=src, dst_ref=dst, send_sem=s_sem.at[k, lax.rem(c, SLOTS)], recv_sem=r_sem.at[k, c], device_id={"tp": to}, device_id_type=MESH
        )

    def y_at(r, n, c):
        return y_ref.at[pl.ds(pl.multiple_of(r, 32), n), pl.ds(pl.multiple_of(c * W, W), W)]

    def p0(c):
        return [remote(send0.at[lax.rem(c, 2)], recv0.at[c], 0, c, p_core)]

    def p1(c):
        s = lax.rem(c, SLOTS)
        return [remote(send1.at[s, 0], recv1.at[c, 0], 1, c, p_x), remote(send1.at[s, 1], recv1.at[c, 1], 2, c, p_y)]

    def p2(c):
        s = lax.rem(c, SLOTS)
        return [remote(send2.at[s, 0], recv2.at[c, 0], 3, c, p_y), remote(send2.at[s, 1], recv2.at[c, 1], 4, c, p_x)]

    def p3(c):
        return [remote(y_at(own1, 32, c), y_at(own1, 32, c), 5, c, p_y), remote(y_at(own2, 32, c), y_at(own2, 32, c), 6, c, p_x)]

    def p4(c):
        return [remote(y_at(base1, 64, c), y_at(base1, 64, c), 7, c, p_x), remote(y_at(base2, 64, c), y_at(base2, 64, c), 8, c, p_y)]

    def p5(c):
        half = 256 * core
        return [remote(y_at(half, 256, c), y_at(half, 256, c), 9, c, p_core)]

    def guard(cond, fn):
        if isinstance(cond, bool):
            if cond:
                fn()
        else:
            pl.when(cond)(fn)

    def drain(make, c):
        def fn():
            for d in make(c - SLOTS):
                d.wait_send()

        guard(c >= SLOTS, fn)

    def start(make, c):
        drain(make, c)
        for d in make(c):
            d.start()

    def stage0(c):
        for d in p0(c):
            d.wait_recv()
        k = lax.rem(c, SLOTS)
        drain(p1, c)
        for h in range(2):
            o = 128 * h
            send1[k, h] = (keep0[lax.rem(c, 2), o : o + 64] + recv0[c, o : o + 64].astype(F32)).astype(BF16)
            keep1[k, h] = keep0[lax.rem(c, 2), o + 64 : o + 128] + recv0[c, o + 64 : o + 128].astype(F32)
        for d in p1(c):
            d.start()

    def stage1(c):
        for d in p1(c):
            d.wait_recv()
        k = lax.rem(c, SLOTS)
        drain(p2, c)
        for h in range(2):
            send2[k, h] = (keep1[k, h, 0:32] + recv1[c, h, 0:32].astype(F32)).astype(BF16)
            keep2[k, h] = keep1[k, h, 32:64] + recv1[c, h, 32:64].astype(F32)
        for d in p2(c):
            d.start()

    def stage2(c):
        for d in p2(c):
            d.wait_recv()
        k = lax.rem(c, SLOTS)
        cols = pl.ds(pl.multiple_of(c * W, W), W)
        for h, r in enumerate((own1, own2)):
            y_ref[pl.ds(pl.multiple_of(r, 32), 32), cols] = (keep2[k, h] + recv2[c, h].astype(F32)).astype(BF16)
        start(p3, c)

    def stage3(c):
        for d in p3(c):
            d.wait_recv()
        start(p4, c)

    def stage4(c):
        for d in p4(c):
            d.wait_recv()
        start(p5, c)

    stages = (stage0, stage1, stage2, stage3, stage4)
    part_k = (ka + km) // PARTS

    def serve(i, q, static):
        for k in (4, 3, 2, 1, 0):
            back, rem = divmod(LAG[k] + PARTS - 1 - q, PARTS)
            if rem == 0:
                guard(i >= back, functools.partial(stages[k], i - back))

    def finish(i, slot, total):
        send0[slot] = total[0:256].astype(BF16)
        keep0[slot] = total[256:512]
        for d in p0(i):
            d.start()

    total = None
    for j in range(n_slices):
        first[j].wait()
        pltpu.make_async_copy(ctx_ref.at[:, pl.ds(0, 1536)], x_v.at[:, pl.ds(j * 1536, 1536)], x_sem.at[j]).wait()
        if j == 0:
            for cp in w_copies(1, 1):
                cp.start()
        piece = jnp.dot(x_v[:, j * 1536 : (j + 1) * 1536], w_v[0, j * 1536 : (j + 1) * 1536], preferred_element_type=F32)
        total = piece if total is None else piece + total
    pl.semaphore_wait(barrier, 3)
    finish(0, 0, total)

    @pl.when(core == 1)
    def _():
        wait_v[...] = jnp.dot(x_v[:, 0:DELAY], w_v[0, 0:DELAY], preferred_element_type=F32)

    def step(i, static):
        slot = i % 2 if static else lax.rem(i, 2)
        for cp in w_copies(i, slot):
            cp.wait()

        def ahead():
            for cp in w_copies(i + 1, 1 - slot):
                cp.start()

        guard(i + 1 < n_chunks, ahead)

        def sent():
            for d in p0(i - 2):
                d.wait_send()

        guard(i >= 2, sent)
        total = None
        for q in range(PARTS):
            piece = jnp.dot(x_v[:, q * part_k : (q + 1) * part_k], w_v[slot, q * part_k : (q + 1) * part_k], preferred_element_type=F32)
            total = piece if total is None else piece + total
            if q == PARTS - 1:
                finish(i, slot, total)
            serve(i, q, static)

    for i in range(1, HEAD):
        step(i, True)

    def looped(i, carry):
        step(i, False)
        return carry

    lax.fori_loop(HEAD, n_chunks, looped, 0)
    for k, back in DRAIN:
        stages[k](n_chunks - back)
    for d in p0(n_chunks - 2) + p0(n_chunks - 1):
        d.wait_send()
    for c in range(n_chunks - SLOTS, n_chunks):
        for make in (p1, p2, p3, p4, p5):
            for d in make(c):
                d.wait_send()
    for c in range(n_chunks):
        for d in p5(c):
            d.wait_recv()


def store(y_ref, o_ref, sem):
    n = y_ref.shape[0] // STORES
    copies = [pltpu.make_async_copy(y_ref.at[pl.ds(j * n, n)], o_ref.at[pl.ds(j * n, n)], sem.at[j]) for j in range(STORES)]
    for cp in copies:
        cp.start()
    for cp in copies:
        cp.wait()


def solution(mesh):
    def device_step(ctx, w_out, act, w_down):
        rows, ka = ctx.shape
        km, cols = w_down.shape
        n = cols // W
        any_ = pl.BlockSpec(memory_space=pl.ANY)
        y = pl.pallas_call(
            functools.partial(kernel, n),
            out_shape=pltpu.VMEM((rows, cols), BF16),
            in_specs=[any_] * 4,
            out_specs=pl.BlockSpec(memory_space=pltpu.VMEM),
            scratch_shapes=[
                pltpu.VMEM((rows, ka + km), BF16),
                pltpu.VMEM((2, ka + km, W), BF16),
                pltpu.VMEM((n, 256, W), BF16),
                pltpu.VMEM((n, 2, 64, W), BF16),
                pltpu.VMEM((n, 2, 32, W), BF16),
                pltpu.VMEM((2, 256, W), BF16),
                pltpu.VMEM((SLOTS, 2, 64, W), BF16),
                pltpu.VMEM((SLOTS, 2, 32, W), BF16),
                pltpu.VMEM((2, 256, W), F32),
                pltpu.VMEM((SLOTS, 2, 64, W), F32),
                pltpu.VMEM((SLOTS, 2, 32, W), F32),
                pltpu.VMEM((rows, W), F32),
                pltpu.SemaphoreType.DMA(((ka + km) // 1536,)),
                pltpu.SemaphoreType.DMA((2, (ka + km) // 1536)),
                pltpu.SemaphoreType.DMA((10, SLOTS)),
                pltpu.SemaphoreType.DMA((10, n)),
            ],
            compiler_params=pltpu.CompilerParams(collective_id=0, has_side_effects=True, vmem_limit_bytes=VMEM_LIMIT),
            cost_estimate=pl.CostEstimate(flops=2 * rows * (ka + km) * cols, bytes_accessed=2 * (ka + km) * cols, transcendentals=0),
        )(ctx, w_out, act, w_down)
        return pl.pallas_call(
            store,
            out_shape=jax.ShapeDtypeStruct((rows, cols), BF16),
            in_specs=[pl.BlockSpec(memory_space=pltpu.VMEM)],
            out_specs=pl.BlockSpec(memory_space=pl.ANY),
            scratch_shapes=[pltpu.SemaphoreType.DMA((STORES,))],
            compiler_params=pltpu.CompilerParams(vmem_limit_bytes=1024 * 1024),
            cost_estimate=pl.CostEstimate(flops=0, bytes_accessed=2 * rows * cols, transcendentals=0),
        )(y)

    return jax.shard_map(
        device_step,
        mesh=mesh,
        in_specs=(P("data", "tp"), P("tp", None), P("data", "tp"), P("tp", None)),
        out_specs=P("data", None),
        check_vma=False,
    )
```

```python
import functools

import jax
import jax.numpy as jnp
from jax import lax
from jax.experimental import pallas as pl
from jax.experimental.pallas import tpu as pltpu
from jax.sharding import PartitionSpec as P

MESH = pl.DeviceIdType.MESH
BF16 = jnp.bfloat16
F32 = jnp.float32

W = 512
PARTS = 1
LAG = (1, 3, 4, 5, 7)
ORDER = (1, 2, 3, 0, 4)
HEAD = 1
SLOTS = 4
STORES = 8
VMEM_LIMIT = 44 * 1024 * 1024
DRAIN = ((4, 7), (0, 1), (1, 3), (2, 4), (3, 5), (4, 6), (1, 2), (1, 1), (2, 3), (3, 4), (4, 5), (2, 2), (2, 1), (3, 3), (4, 4), (3, 2), (3, 1), (4, 3), (4, 2), (4, 1))


def kernel(n_chunks, ctx_ref, wo_ref, act_ref, wd_ref, y_ref, x_v, w_v, recv0, recv1, recv2, send0, send1, send2, keep0, keep1, keep2, x_sem, w_sem, s_sem, r_sem):
    me = lax.axis_index("tp")
    core = lax.rem(me, 2)
    cx = lax.rem(me // 2, 2)
    cy = me // 4
    p_core = me + 1 - 2 * core
    p_x = me + 2 - 4 * cx
    p_y = me + 4 - 8 * cy
    ka = ctx_ref.shape[1]
    km = act_ref.shape[1]

    def half_rows(c):
        base = 256 * c
        h1 = [
            base + 64 * (1 - cx) + 32 * (1 - cy),
            base + 64 * (1 - cx) + 32 * cy,
            base + 64 * cx + 32 * (1 - cy),
            base + 64 * cx + 32 * cy,
        ]
        base = base + 128
        h2 = [
            base + 64 * (1 - cy) + 32 * (1 - cx),
            base + 64 * (1 - cy) + 32 * cx,
            base + 64 * cy + 32 * (1 - cx),
            base + 64 * cy + 32 * cx,
        ]
        return h1 + h2

    rows = half_rows(1 - core) + half_rows(core)
    base1 = 256 * core + 64 * cx
    base2 = 256 * core + 128 + 64 * cy
    own1 = base1 + 32 * cy
    own2 = base2 + 32 * cx

    def w_copies(c, slot):
        cols = pl.ds(pl.multiple_of(c * W, W), W)
        out = []
        for j in range(ka // 1536):
            out.append(pltpu.make_async_copy(wo_ref.at[pl.ds(j * 1536, 1536), cols], w_v.at[slot, pl.ds(j * 1536, 1536)], w_sem.at[slot, len(out)]))
        for j in range(km // 1536):
            out.append(pltpu.make_async_copy(wd_ref.at[pl.ds(j * 1536, 1536), cols], w_v.at[slot, pl.ds(ka + j * 1536, 1536)], w_sem.at[slot, len(out)]))
        return out

    def x_copies(j):
        out = []
        for b, r in enumerate(rows):
            r = pl.multiple_of(r, 32)
            src = ctx_ref.at[pl.ds(r, 32), pl.ds(j * 1536, 1536)] if j * 1536 < ka else act_ref.at[pl.ds(r, 32), pl.ds(j * 1536 - ka, 1536)]
            out.append(pltpu.make_async_copy(src, x_v.at[pl.ds(32 * b, 32), pl.ds(j * 1536, 1536)], x_sem.at[j]))
        return out

    barrier = pltpu.get_barrier_semaphore()
    for p in (p_core, p_x, p_y):
        pl.semaphore_signal(barrier, inc=1, device_id={"tp": p}, device_id_type=MESH)
    n_slices = (ka + km) // 1536
    first = w_copies(0, 0)
    for j in range(n_slices):
        first[j].start()
        for cp in x_copies(j):
            cp.start()

    def remote(src, dst, k, c, to):
        return pltpu.make_async_remote_copy(
            src_ref=src, dst_ref=dst, send_sem=s_sem.at[k, lax.rem(c, SLOTS)], recv_sem=r_sem.at[k, c], device_id={"tp": to}, device_id_type=MESH
        )

    def y_at(r, n, c):
        return y_ref.at[pl.ds(pl.multiple_of(r, 32), n), pl.ds(pl.multiple_of(c * W, W), W)]

    def p0(c):
        return [remote(send0.at[lax.rem(c, 2)], recv0.at[c], 0, c, p_core)]

    def p1(c):
        s = lax.rem(c, SLOTS)
        return [remote(send1.at[s, 0], recv1.at[c, 0], 1, c, p_x), remote(send1.at[s, 1], recv1.at[c, 1], 2, c, p_y)]

    def p2(c):
        s = lax.rem(c, SLOTS)
        return [remote(send2.at[s, 0], recv2.at[c, 0], 3, c, p_y), remote(send2.at[s, 1], recv2.at[c, 1], 4, c, p_x)]

    def p3(c):
        return [remote(y_at(own1, 32, c), y_at(own1, 32, c), 5, c, p_y), remote(y_at(own2, 32, c), y_at(own2, 32, c), 6, c, p_x)]

    def p4(c):
        return [remote(y_at(base1, 64, c), y_at(base1, 64, c), 7, c, p_x), remote(y_at(base2, 64, c), y_at(base2, 64, c), 8, c, p_y)]

    def p5(c):
        half = 256 * core
        return [remote(y_at(half, 256, c), y_at(half, 256, c), 9, c, p_core)]

    def guard(cond, fn):
        if isinstance(cond, bool):
            if cond:
                fn()
        else:
            pl.when(cond)(fn)

    def drain(make, c):
        def fn():
            for d in make(c - SLOTS):
                d.wait_send()

        guard(c >= SLOTS, fn)

    def start(make, c):
        drain(make, c)
        for d in make(c):
            d.start()

    def stage0(c):
        for d in p0(c):
            d.wait_recv()
        k = lax.rem(c, SLOTS)
        drain(p1, c)
        for h in range(2):
            o = 128 * h
            send1[k, h] = (keep0[lax.rem(c, 2), o : o + 64] + recv0[c, o : o + 64].astype(F32)).astype(BF16)
            keep1[k, h] = keep0[lax.rem(c, 2), o + 64 : o + 128] + recv0[c, o + 64 : o + 128].astype(F32)
        for d in p1(c):
            d.start()

    def stage1(c):
        for d in p1(c):
            d.wait_recv()
        k = lax.rem(c, SLOTS)
        drain(p2, c)
        for h in range(2):
            send2[k, h] = (keep1[k, h, 0:32] + recv1[c, h, 0:32].astype(F32)).astype(BF16)
            keep2[k, h] = keep1[k, h, 32:64] + recv1[c, h, 32:64].astype(F32)
        for d in p2(c):
            d.start()

    def stage2(c):
        for d in p2(c):
            d.wait_recv()
        k = lax.rem(c, SLOTS)
        cols = pl.ds(pl.multiple_of(c * W, W), W)
        for h, r in enumerate((own1, own2)):
            y_ref[pl.ds(pl.multiple_of(r, 32), 32), cols] = (keep2[k, h] + recv2[c, h].astype(F32)).astype(BF16)
        start(p3, c)

    def stage3(c):
        for d in p3(c):
            d.wait_recv()
        start(p4, c)

    def stage4(c):
        for d in p4(c):
            d.wait_recv()
        start(p5, c)

    stages = (stage0, stage1, stage2, stage3, stage4)
    part_k = (ka + km) // PARTS

    def serve(i, q, static):
        for k in ORDER:
            back, rem = divmod(LAG[k] + PARTS - 1 - q, PARTS)
            if rem == 0:
                guard(i >= back, functools.partial(stages[k], i - back))

    def finish(i, slot, total):
        send0[slot] = total[0:256].astype(BF16)
        keep0[slot] = total[256:512]
        for d in p0(i):
            d.start()

    total = None
    for j in range(n_slices):
        first[j].wait()
        pltpu.make_async_copy(ctx_ref.at[:, pl.ds(0, 1536)], x_v.at[:, pl.ds(j * 1536, 1536)], x_sem.at[j]).wait()
        if j == 0:
            for cp in w_copies(1, 1):
                cp.start()
        piece = jnp.dot(x_v[:, j * 1536 : (j + 1) * 1536], w_v[0, j * 1536 : (j + 1) * 1536], preferred_element_type=F32)
        total = piece if total is None else piece + total
    pl.semaphore_wait(barrier, 3)
    finish(0, 0, total)

    def step(i, static):
        slot = i % 2 if static else lax.rem(i, 2)
        for cp in w_copies(i, slot):
            cp.wait()

        def ahead():
            for cp in w_copies(i + 1, 1 - slot):
                cp.start()

        guard(i + 1 < n_chunks, ahead)

        def sent():
            for d in p0(i - 2):
                d.wait_send()

        guard(i >= 2, sent)
        total = None
        for q in range(PARTS):
            piece = jnp.dot(x_v[:, q * part_k : (q + 1) * part_k], w_v[slot, q * part_k : (q + 1) * part_k], preferred_element_type=F32)
            total = piece if total is None else piece + total
            if q == PARTS - 1:
                finish(i, slot, total)
            serve(i, q, static)

    for i in range(1, HEAD):
        step(i, True)

    def looped(i, carry):
        step(i, False)
        return carry

    lax.fori_loop(HEAD, n_chunks, looped, 0)
    for k, back in DRAIN:
        stages[k](n_chunks - back)
    for d in p0(n_chunks - 2) + p0(n_chunks - 1):
        d.wait_send()
    for c in range(n_chunks - SLOTS, n_chunks):
        for make in (p1, p2, p3, p4, p5):
            for d in make(c):
                d.wait_send()
    for c in range(n_chunks):
        for d in p5(c):
            d.wait_recv()


def store(y_ref, o_ref, sem):
    n = y_ref.shape[0] // STORES
    copies = [pltpu.make_async_copy(y_ref.at[pl.ds(j * n, n)], o_ref.at[pl.ds(j * n, n)], sem.at[j]) for j in range(STORES)]
    for cp in copies:
        cp.start()
    for cp in copies:
        cp.wait()


def solution(mesh):
    def device_step(ctx, w_out, act, w_down):
        rows, ka = ctx.shape
        km, cols = w_down.shape
        n = cols // W
        any_ = pl.BlockSpec(memory_space=pl.ANY)
        y = pl.pallas_call(
            functools.partial(kernel, n),
            out_shape=pltpu.VMEM((rows, cols), BF16),
            in_specs=[any_] * 4,
            out_specs=pl.BlockSpec(memory_space=pltpu.VMEM),
            scratch_shapes=[
                pltpu.VMEM((rows, ka + km), BF16),
                pltpu.VMEM((2, ka + km, W), BF16),
                pltpu.VMEM((n, 256, W), BF16),
                pltpu.VMEM((n, 2, 64, W), BF16),
                pltpu.VMEM((n, 2, 32, W), BF16),
                pltpu.VMEM((2, 256, W), BF16),
                pltpu.VMEM((SLOTS, 2, 64, W), BF16),
                pltpu.VMEM((SLOTS, 2, 32, W), BF16),
                pltpu.VMEM((2, 256, W), F32),
                pltpu.VMEM((SLOTS, 2, 64, W), F32),
                pltpu.VMEM((SLOTS, 2, 32, W), F32),
                pltpu.SemaphoreType.DMA(((ka + km) // 1536,)),
                pltpu.SemaphoreType.DMA((2, (ka + km) // 1536)),
                pltpu.SemaphoreType.DMA((10, SLOTS)),
                pltpu.SemaphoreType.DMA((10, n)),
            ],
            compiler_params=pltpu.CompilerParams(collective_id=0, has_side_effects=True, vmem_limit_bytes=VMEM_LIMIT),
            cost_estimate=pl.CostEstimate(flops=2 * rows * (ka + km) * cols, bytes_accessed=2 * (ka + km) * cols, transcendentals=0),
        )(ctx, w_out, act, w_down)
        return pl.pallas_call(
            store,
            out_shape=jax.ShapeDtypeStruct((rows, cols), BF16),
            in_specs=[pl.BlockSpec(memory_space=pltpu.VMEM)],
            out_specs=pl.BlockSpec(memory_space=pl.ANY),
            scratch_shapes=[pltpu.SemaphoreType.DMA((STORES,))],
            compiler_params=pltpu.CompilerParams(vmem_limit_bytes=1024 * 1024),
            cost_estimate=pl.CostEstimate(flops=0, bytes_accessed=2 * rows * cols, transcendentals=0),
        )(y)

    return jax.shard_map(
        device_step,
        mesh=mesh,
        in_specs=(P("data", "tp"), P("tp", None), P("data", "tp"), P("tp", None)),
        out_specs=P("data", None),
        check_vma=False,
    )
```

```python
import functools

import jax
import jax.numpy as jnp
from jax import lax
from jax.experimental import pallas as pl
from jax.experimental.pallas import tpu as pltpu
from jax.sharding import PartitionSpec as P

MESH = pl.DeviceIdType.MESH
BF16 = jnp.bfloat16
F32 = jnp.float32

W = 512
EARLY = 1280
LAG = (0, 2, 3, 4, 6)
ORDER = (1, 2, 3, 0, 4)
HEAD = 1
SLOTS = 4
STORES = 8
VMEM_LIMIT = 44 * 1024 * 1024
DRAIN = ((4, 6), (1, 2), (2, 3), (3, 4), (4, 5), (1, 1), (2, 2), (3, 3), (4, 4), (2, 1), (3, 2), (4, 3), (3, 1), (4, 2), (4, 1))


def kernel(n_chunks, ctx_ref, wo_ref, act_ref, wd_ref, y_ref, x_v, w_v, recv0, recv1, recv2, send0, send1, send2, keep0, keep1, keep2, x_sem, w_sem, s_sem, r_sem):
    me = lax.axis_index("tp")
    core = lax.rem(me, 2)
    cx = lax.rem(me // 2, 2)
    cy = me // 4
    p_core = me + 1 - 2 * core
    p_x = me + 2 - 4 * cx
    p_y = me + 4 - 8 * cy
    ka = ctx_ref.shape[1]
    km = act_ref.shape[1]

    def half_rows(c):
        base = 256 * c
        h1 = [
            base + 64 * (1 - cx) + 32 * (1 - cy),
            base + 64 * (1 - cx) + 32 * cy,
            base + 64 * cx + 32 * (1 - cy),
            base + 64 * cx + 32 * cy,
        ]
        base = base + 128
        h2 = [
            base + 64 * (1 - cy) + 32 * (1 - cx),
            base + 64 * (1 - cy) + 32 * cx,
            base + 64 * cy + 32 * (1 - cx),
            base + 64 * cy + 32 * cx,
        ]
        return h1 + h2

    rows = half_rows(1 - core) + half_rows(core)
    base1 = 256 * core + 64 * cx
    base2 = 256 * core + 128 + 64 * cy
    own1 = base1 + 32 * cy
    own2 = base2 + 32 * cx

    def w_copies(c, slot):
        cols = pl.ds(pl.multiple_of(c * W, W), W)
        out = []
        for j in range(ka // 1536):
            out.append(pltpu.make_async_copy(wo_ref.at[pl.ds(j * 1536, 1536), cols], w_v.at[slot, pl.ds(j * 1536, 1536)], w_sem.at[slot, len(out)]))
        for j in range(km // 1536):
            out.append(pltpu.make_async_copy(wd_ref.at[pl.ds(j * 1536, 1536), cols], w_v.at[slot, pl.ds(ka + j * 1536, 1536)], w_sem.at[slot, len(out)]))
        return out

    def x_copies(j):
        out = []
        for b, r in enumerate(rows):
            r = pl.multiple_of(r, 32)
            src = ctx_ref.at[pl.ds(r, 32), pl.ds(j * 1536, 1536)] if j * 1536 < ka else act_ref.at[pl.ds(r, 32), pl.ds(j * 1536 - ka, 1536)]
            out.append(pltpu.make_async_copy(src, x_v.at[pl.ds(32 * b, 32), pl.ds(j * 1536, 1536)], x_sem.at[j]))
        return out

    barrier = pltpu.get_barrier_semaphore()
    for p in (p_core, p_x, p_y):
        pl.semaphore_signal(barrier, inc=1, device_id={"tp": p}, device_id_type=MESH)
    n_slices = (ka + km) // 1536
    first = w_copies(0, 0)
    for j in range(n_slices):
        first[j].start()
        for cp in x_copies(j):
            cp.start()

    def remote(src, dst, k, c, to):
        return pltpu.make_async_remote_copy(
            src_ref=src, dst_ref=dst, send_sem=s_sem.at[k, lax.rem(c, SLOTS)], recv_sem=r_sem.at[k, c], device_id={"tp": to}, device_id_type=MESH
        )

    def y_at(r, n, c):
        return y_ref.at[pl.ds(pl.multiple_of(r, 32), n), pl.ds(pl.multiple_of(c * W, W), W)]

    def p0(c):
        return [remote(send0.at[lax.rem(c, 2)], recv0.at[c], 0, c, p_core)]

    def p1(c):
        s = lax.rem(c, SLOTS)
        return [remote(send1.at[s, 0], recv1.at[c, 0], 1, c, p_x), remote(send1.at[s, 1], recv1.at[c, 1], 2, c, p_y)]

    def p2(c):
        s = lax.rem(c, SLOTS)
        return [remote(send2.at[s, 0], recv2.at[c, 0], 3, c, p_y), remote(send2.at[s, 1], recv2.at[c, 1], 4, c, p_x)]

    def p3(c):
        return [remote(y_at(own1, 32, c), y_at(own1, 32, c), 5, c, p_y), remote(y_at(own2, 32, c), y_at(own2, 32, c), 6, c, p_x)]

    def p4(c):
        return [remote(y_at(base1, 64, c), y_at(base1, 64, c), 7, c, p_x), remote(y_at(base2, 64, c), y_at(base2, 64, c), 8, c, p_y)]

    def p5(c):
        half = 256 * core
        return [remote(y_at(half, 256, c), y_at(half, 256, c), 9, c, p_core)]

    def guard(cond, fn):
        if isinstance(cond, bool):
            if cond:
                fn()
        else:
            pl.when(cond)(fn)

    def drain(make, c):
        def fn():
            for d in make(c - SLOTS):
                d.wait_send()

        guard(c >= SLOTS, fn)

    def start(make, c):
        drain(make, c)
        for d in make(c):
            d.start()

    def stage0(c):
        for d in p0(c):
            d.wait_recv()
        k = lax.rem(c, SLOTS)
        drain(p1, c)
        for h in range(2):
            o = 128 * h
            send1[k, h] = (keep0[lax.rem(c, 2), o : o + 64] + recv0[c, o : o + 64].astype(F32)).astype(BF16)
            keep1[k, h] = keep0[lax.rem(c, 2), o + 64 : o + 128] + recv0[c, o + 64 : o + 128].astype(F32)
        for d in p1(c):
            d.start()

    def stage1(c):
        for d in p1(c):
            d.wait_recv()
        k = lax.rem(c, SLOTS)
        drain(p2, c)
        for h in range(2):
            send2[k, h] = (keep1[k, h, 0:32] + recv1[c, h, 0:32].astype(F32)).astype(BF16)
            keep2[k, h] = keep1[k, h, 32:64] + recv1[c, h, 32:64].astype(F32)
        for d in p2(c):
            d.start()

    def stage2(c):
        for d in p2(c):
            d.wait_recv()
        k = lax.rem(c, SLOTS)
        cols = pl.ds(pl.multiple_of(c * W, W), W)
        for h, r in enumerate((own1, own2)):
            y_ref[pl.ds(pl.multiple_of(r, 32), 32), cols] = (keep2[k, h] + recv2[c, h].astype(F32)).astype(BF16)
        start(p3, c)

    def stage3(c):
        for d in p3(c):
            d.wait_recv()
        start(p4, c)

    def stage4(c):
        for d in p4(c):
            d.wait_recv()
        start(p5, c)

    stages = (stage0, stage1, stage2, stage3, stage4)
    def serve(i):
        for k in ORDER:
            back = LAG[k]
            guard(i >= back, functools.partial(stages[k], i - back))

    def push_out(i, slot, theirs):
        send0[slot] = theirs.astype(BF16)
        for d in p0(i):
            d.start()

    total = None
    for j in range(n_slices):
        first[j].wait()
        pltpu.make_async_copy(ctx_ref.at[:, pl.ds(0, 1536)], x_v.at[:, pl.ds(j * 1536, 1536)], x_sem.at[j]).wait()
        if j == 0:
            for cp in w_copies(1, 1):
                cp.start()
        piece = jnp.dot(x_v[:, j * 1536 : (j + 1) * 1536], w_v[0, j * 1536 : (j + 1) * 1536], preferred_element_type=F32)
        total = piece if total is None else piece + total
    pl.semaphore_wait(barrier, 3)
    push_out(0, 0, total[0:256])
    keep0[0] = total[256:512]
    serve(0)

    def step(i, static):
        slot = i % 2 if static else lax.rem(i, 2)
        for cp in w_copies(i, slot):
            cp.wait()

        def ahead():
            for cp in w_copies(i + 1, 1 - slot):
                cp.start()

        guard(i + 1 < n_chunks, ahead)

        def sent():
            for d in p0(i - 2):
                d.wait_send()

        guard(i >= 2, sent)
        theirs = jnp.dot(x_v[0:256], w_v[slot], preferred_element_type=F32)
        early = jnp.dot(x_v[256:512, 0:EARLY], w_v[slot, 0:EARLY], preferred_element_type=F32)
        push_out(i, slot, theirs)
        keep0[slot] = jnp.dot(x_v[256:512, EARLY:], w_v[slot, EARLY:], preferred_element_type=F32) + early
        serve(i)

    for i in range(1, HEAD):
        step(i, True)

    def looped(i, carry):
        step(i, False)
        return carry

    lax.fori_loop(HEAD, n_chunks, looped, 0)
    for k, back in DRAIN:
        stages[k](n_chunks - back)
    for d in p0(n_chunks - 2) + p0(n_chunks - 1):
        d.wait_send()
    for c in range(n_chunks - SLOTS, n_chunks):
        for make in (p1, p2, p3, p4, p5):
            for d in make(c):
                d.wait_send()
    for c in range(n_chunks):
        for d in p5(c):
            d.wait_recv()


def store(y_ref, o_ref, sem):
    n = y_ref.shape[0] // STORES
    copies = [pltpu.make_async_copy(y_ref.at[pl.ds(j * n, n)], o_ref.at[pl.ds(j * n, n)], sem.at[j]) for j in range(STORES)]
    for cp in copies:
        cp.start()
    for cp in copies:
        cp.wait()


def solution(mesh):
    def device_step(ctx, w_out, act, w_down):
        rows, ka = ctx.shape
        km, cols = w_down.shape
        n = cols // W
        any_ = pl.BlockSpec(memory_space=pl.ANY)
        y = pl.pallas_call(
            functools.partial(kernel, n),
            out_shape=pltpu.VMEM((rows, cols), BF16),
            in_specs=[any_] * 4,
            out_specs=pl.BlockSpec(memory_space=pltpu.VMEM),
            scratch_shapes=[
                pltpu.VMEM((rows, ka + km), BF16),
                pltpu.VMEM((2, ka + km, W), BF16),
                pltpu.VMEM((n, 256, W), BF16),
                pltpu.VMEM((n, 2, 64, W), BF16),
                pltpu.VMEM((n, 2, 32, W), BF16),
                pltpu.VMEM((2, 256, W), BF16),
                pltpu.VMEM((SLOTS, 2, 64, W), BF16),
                pltpu.VMEM((SLOTS, 2, 32, W), BF16),
                pltpu.VMEM((2, 256, W), F32),
                pltpu.VMEM((SLOTS, 2, 64, W), F32),
                pltpu.VMEM((SLOTS, 2, 32, W), F32),
                pltpu.SemaphoreType.DMA(((ka + km) // 1536,)),
                pltpu.SemaphoreType.DMA((2, (ka + km) // 1536)),
                pltpu.SemaphoreType.DMA((10, SLOTS)),
                pltpu.SemaphoreType.DMA((10, n)),
            ],
            compiler_params=pltpu.CompilerParams(collective_id=0, has_side_effects=True, vmem_limit_bytes=VMEM_LIMIT),
            cost_estimate=pl.CostEstimate(flops=2 * rows * (ka + km) * cols, bytes_accessed=2 * (ka + km) * cols, transcendentals=0),
        )(ctx, w_out, act, w_down)
        return pl.pallas_call(
            store,
            out_shape=jax.ShapeDtypeStruct((rows, cols), BF16),
            in_specs=[pl.BlockSpec(memory_space=pltpu.VMEM)],
            out_specs=pl.BlockSpec(memory_space=pl.ANY),
            scratch_shapes=[pltpu.SemaphoreType.DMA((STORES,))],
            compiler_params=pltpu.CompilerParams(vmem_limit_bytes=1024 * 1024),
            cost_estimate=pl.CostEstimate(flops=0, bytes_accessed=2 * rows * cols, transcendentals=0),
        )(y)

    return jax.shard_map(
        device_step,
        mesh=mesh,
        in_specs=(P("data", "tp"), P("tp", None), P("data", "tp"), P("tp", None)),
        out_specs=P("data", None),
        check_vma=False,
    )
```

```python
import functools

import jax
import jax.numpy as jnp
from jax import lax
from jax.experimental import pallas as pl
from jax.experimental.pallas import tpu as pltpu
from jax.sharding import PartitionSpec as P

MESH = pl.DeviceIdType.MESH
BF16 = jnp.bfloat16
F32 = jnp.float32

W = 512
EARLY = 1280
LAG = (0, 1, 2, 4, 6)
ORDER = (0, 1, 3, 2, 4)
HEAD = 1
SLOTS = 4
STORES = 8
VMEM_LIMIT = 44 * 1024 * 1024
DRAIN = ((4, 6), (3, 4), (1, 1), (2, 2), (4, 5), (3, 3), (4, 4), (2, 1), (3, 2), (4, 3), (3, 1), (4, 2), (4, 1))


def kernel(n_chunks, ctx_ref, wo_ref, act_ref, wd_ref, y_ref, x_v, w_v, recv0, recv1, recv2, send0, send1, send2, keep0, keep1, keep2, x_sem, w_sem, s_sem, r_sem):
    me = lax.axis_index("tp")
    core = lax.rem(me, 2)
    cx = lax.rem(me // 2, 2)
    cy = me // 4
    p_core = me + 1 - 2 * core
    p_x = me + 2 - 4 * cx
    p_y = me + 4 - 8 * cy
    ka = ctx_ref.shape[1]
    km = act_ref.shape[1]

    def half_rows(c):
        base = 256 * c
        h1 = [
            base + 64 * (1 - cx) + 32 * (1 - cy),
            base + 64 * (1 - cx) + 32 * cy,
            base + 64 * cx + 32 * (1 - cy),
            base + 64 * cx + 32 * cy,
        ]
        base = base + 128
        h2 = [
            base + 64 * (1 - cy) + 32 * (1 - cx),
            base + 64 * (1 - cy) + 32 * cx,
            base + 64 * cy + 32 * (1 - cx),
            base + 64 * cy + 32 * cx,
        ]
        return h1 + h2

    rows = half_rows(1 - core) + half_rows(core)
    base1 = 256 * core + 64 * cx
    base2 = 256 * core + 128 + 64 * cy
    own1 = base1 + 32 * cy
    own2 = base2 + 32 * cx

    def w_copies(c, slot):
        cols = pl.ds(pl.multiple_of(c * W, W), W)
        out = []
        for j in range(ka // 1536):
            out.append(pltpu.make_async_copy(wo_ref.at[pl.ds(j * 1536, 1536), cols], w_v.at[slot, pl.ds(j * 1536, 1536)], w_sem.at[slot, len(out)]))
        for j in range(km // 1536):
            out.append(pltpu.make_async_copy(wd_ref.at[pl.ds(j * 1536, 1536), cols], w_v.at[slot, pl.ds(ka + j * 1536, 1536)], w_sem.at[slot, len(out)]))
        return out

    def x_copies(j):
        out = []
        for b, r in enumerate(rows):
            r = pl.multiple_of(r, 32)
            src = ctx_ref.at[pl.ds(r, 32), pl.ds(j * 1536, 1536)] if j * 1536 < ka else act_ref.at[pl.ds(r, 32), pl.ds(j * 1536 - ka, 1536)]
            out.append(pltpu.make_async_copy(src, x_v.at[pl.ds(32 * b, 32), pl.ds(j * 1536, 1536)], x_sem.at[j]))
        return out

    barrier = pltpu.get_barrier_semaphore()
    for p in (p_core, p_x, p_y):
        pl.semaphore_signal(barrier, inc=1, device_id={"tp": p}, device_id_type=MESH)
    n_slices = (ka + km) // 1536
    first = w_copies(0, 0)
    for j in range(n_slices):
        first[j].start()
        for cp in x_copies(j):
            cp.start()

    def remote(src, dst, k, c, to):
        return pltpu.make_async_remote_copy(
            src_ref=src, dst_ref=dst, send_sem=s_sem.at[k, lax.rem(c, SLOTS)], recv_sem=r_sem.at[k, c], device_id={"tp": to}, device_id_type=MESH
        )

    def y_at(r, n, c):
        return y_ref.at[pl.ds(pl.multiple_of(r, 32), n), pl.ds(pl.multiple_of(c * W, W), W)]

    def p0(c):
        return [remote(send0.at[lax.rem(c, 2)], recv0.at[c], 0, c, p_core)]

    def p1(c):
        s = lax.rem(c, SLOTS)
        return [remote(send1.at[s, 0], recv1.at[c, 0], 1, c, p_x), remote(send1.at[s, 1], recv1.at[c, 1], 2, c, p_y)]

    def p2(c):
        s = lax.rem(c, SLOTS)
        return [remote(send2.at[s, 0], recv2.at[c, 0], 3, c, p_y), remote(send2.at[s, 1], recv2.at[c, 1], 4, c, p_x)]

    def p3(c):
        return [remote(y_at(own1, 32, c), y_at(own1, 32, c), 5, c, p_y), remote(y_at(own2, 32, c), y_at(own2, 32, c), 6, c, p_x)]

    def p4(c):
        return [remote(y_at(base1, 64, c), y_at(base1, 64, c), 7, c, p_x), remote(y_at(base2, 64, c), y_at(base2, 64, c), 8, c, p_y)]

    def p5(c):
        half = 256 * core
        return [remote(y_at(half, 256, c), y_at(half, 256, c), 9, c, p_core)]

    def guard(cond, fn):
        if isinstance(cond, bool):
            if cond:
                fn()
        else:
            pl.when(cond)(fn)

    def drain(make, c):
        def fn():
            for d in make(c - SLOTS):
                d.wait_send()

        guard(c >= SLOTS, fn)

    def start(make, c):
        drain(make, c)
        for d in make(c):
            d.start()

    def stage0(c):
        for d in p0(c):
            d.wait_recv()
        k = lax.rem(c, SLOTS)
        drain(p1, c)
        for h in range(2):
            o = 128 * h
            send1[k, h] = (keep0[lax.rem(c, 2), o : o + 64] + recv0[c, o : o + 64].astype(F32)).astype(BF16)
            keep1[k, h] = keep0[lax.rem(c, 2), o + 64 : o + 128] + recv0[c, o + 64 : o + 128].astype(F32)
        for d in p1(c):
            d.start()

    def stage1(c):
        for d in p1(c):
            d.wait_recv()
        k = lax.rem(c, SLOTS)
        drain(p2, c)
        for h in range(2):
            send2[k, h] = (keep1[k, h, 0:32] + recv1[c, h, 0:32].astype(F32)).astype(BF16)
            keep2[k, h] = keep1[k, h, 32:64] + recv1[c, h, 32:64].astype(F32)
        for d in p2(c):
            d.start()

    def stage2(c):
        for d in p2(c):
            d.wait_recv()
        k = lax.rem(c, SLOTS)
        cols = pl.ds(pl.multiple_of(c * W, W), W)
        for h, r in enumerate((own1, own2)):
            y_ref[pl.ds(pl.multiple_of(r, 32), 32), cols] = (keep2[k, h] + recv2[c, h].astype(F32)).astype(BF16)
        start(p3, c)

    def stage3(c):
        for d in p3(c):
            d.wait_recv()
        start(p4, c)

    def stage4(c):
        for d in p4(c):
            d.wait_recv()
        start(p5, c)

    stages = (stage0, stage1, stage2, stage3, stage4)
    def serve(i):
        for k in ORDER:
            back = LAG[k]
            guard(i >= back, functools.partial(stages[k], i - back))

    def push_out(i, slot, theirs):
        send0[slot] = theirs.astype(BF16)
        for d in p0(i):
            d.start()

    total = None
    for j in range(n_slices):
        first[j].wait()
        pltpu.make_async_copy(ctx_ref.at[:, pl.ds(0, 1536)], x_v.at[:, pl.ds(j * 1536, 1536)], x_sem.at[j]).wait()
        if j == 0:
            for cp in w_copies(1, 1):
                cp.start()
        piece = jnp.dot(x_v[:, j * 1536 : (j + 1) * 1536], w_v[0, j * 1536 : (j + 1) * 1536], preferred_element_type=F32)
        total = piece if total is None else piece + total
    pl.semaphore_wait(barrier, 3)
    push_out(0, 0, total[0:256])
    keep0[0] = total[256:512]
    serve(0)

    def step(i, static):
        slot = i % 2 if static else lax.rem(i, 2)
        for cp in w_copies(i, slot):
            cp.wait()

        def ahead():
            for cp in w_copies(i + 1, 1 - slot):
                cp.start()

        guard(i + 1 < n_chunks, ahead)

        def sent():
            for d in p0(i - 2):
                d.wait_send()

        guard(i >= 2, sent)
        theirs = jnp.dot(x_v[0:256], w_v[slot], preferred_element_type=F32)
        early = jnp.dot(x_v[256:512, 0:EARLY], w_v[slot, 0:EARLY], preferred_element_type=F32)
        push_out(i, slot, theirs)
        keep0[slot] = jnp.dot(x_v[256:512, EARLY:], w_v[slot, EARLY:], preferred_element_type=F32) + early
        serve(i)

    for i in range(1, HEAD):
        step(i, True)

    def looped(i, carry):
        step(i, False)
        return carry

    lax.fori_loop(HEAD, n_chunks, looped, 0)
    for k, back in DRAIN:
        stages[k](n_chunks - back)
    for d in p0(n_chunks - 2) + p0(n_chunks - 1):
        d.wait_send()
    for c in range(n_chunks - SLOTS, n_chunks):
        for make in (p1, p2, p3, p4, p5):
            for d in make(c):
                d.wait_send()
    for c in range(n_chunks):
        for d in p5(c):
            d.wait_recv()


def store(y_ref, o_ref, sem):
    n = y_ref.shape[0] // STORES
    copies = [pltpu.make_async_copy(y_ref.at[pl.ds(j * n, n)], o_ref.at[pl.ds(j * n, n)], sem.at[j]) for j in range(STORES)]
    for cp in copies:
        cp.start()
    for cp in copies:
        cp.wait()


def solution(mesh):
    def device_step(ctx, w_out, act, w_down):
        rows, ka = ctx.shape
        km, cols = w_down.shape
        n = cols // W
        any_ = pl.BlockSpec(memory_space=pl.ANY)
        y = pl.pallas_call(
            functools.partial(kernel, n),
            out_shape=pltpu.VMEM((rows, cols), BF16),
            in_specs=[any_] * 4,
            out_specs=pl.BlockSpec(memory_space=pltpu.VMEM),
            scratch_shapes=[
                pltpu.VMEM((rows, ka + km), BF16),
                pltpu.VMEM((2, ka + km, W), BF16),
                pltpu.VMEM((n, 256, W), BF16),
                pltpu.VMEM((n, 2, 64, W), BF16),
                pltpu.VMEM((n, 2, 32, W), BF16),
                pltpu.VMEM((2, 256, W), BF16),
                pltpu.VMEM((SLOTS, 2, 64, W), BF16),
                pltpu.VMEM((SLOTS, 2, 32, W), BF16),
                pltpu.VMEM((2, 256, W), F32),
                pltpu.VMEM((SLOTS, 2, 64, W), F32),
                pltpu.VMEM((SLOTS, 2, 32, W), F32),
                pltpu.SemaphoreType.DMA(((ka + km) // 1536,)),
                pltpu.SemaphoreType.DMA((2, (ka + km) // 1536)),
                pltpu.SemaphoreType.DMA((10, SLOTS)),
                pltpu.SemaphoreType.DMA((10, n)),
            ],
            compiler_params=pltpu.CompilerParams(collective_id=0, has_side_effects=True, vmem_limit_bytes=VMEM_LIMIT),
            cost_estimate=pl.CostEstimate(flops=2 * rows * (ka + km) * cols, bytes_accessed=2 * (ka + km) * cols, transcendentals=0),
        )(ctx, w_out, act, w_down)
        return pl.pallas_call(
            store,
            out_shape=jax.ShapeDtypeStruct((rows, cols), BF16),
            in_specs=[pl.BlockSpec(memory_space=pltpu.VMEM)],
            out_specs=pl.BlockSpec(memory_space=pl.ANY),
            scratch_shapes=[pltpu.SemaphoreType.DMA((STORES,))],
            compiler_params=pltpu.CompilerParams(vmem_limit_bytes=1024 * 1024),
            cost_estimate=pl.CostEstimate(flops=0, bytes_accessed=2 * rows * cols, transcendentals=0),
        )(y)

    return jax.shard_map(
        device_step,
        mesh=mesh,
        in_specs=(P("data", "tp"), P("tp", None), P("data", "tp"), P("tp", None)),
        out_specs=P("data", None),
        check_vma=False,
    )
```

```python
import functools

import jax
import jax.numpy as jnp
from jax import lax
from jax.experimental import pallas as pl
from jax.experimental.pallas import tpu as pltpu
from jax.sharding import PartitionSpec as P

MESH = pl.DeviceIdType.MESH
BF16 = jnp.bfloat16
F32 = jnp.float32

W = 512
EARLY = 1280
LAG = (0, 1, 3, 4, 6)
ORDER = (0, 2, 1, 3, 4)
HEAD = 1
SLOTS = 4
STORES = 8
VMEM_LIMIT = 44 * 1024 * 1024
DRAIN = ((2, 3), (4, 6), (1, 1), (3, 4), (2, 2), (4, 5), (3, 3), (2, 1), (4, 4), (3, 2), (4, 3), (3, 1), (4, 2), (4, 1))


def kernel(n_chunks, ctx_ref, wo_ref, act_ref, wd_ref, y_ref, x_v, w_v, recv0, recv1, recv2, send0, send1, send2, keep0, keep1, keep2, x_sem, w_sem, s_sem, r_sem):
    me = lax.axis_index("tp")
    core = lax.rem(me, 2)
    cx = lax.rem(me // 2, 2)
    cy = me // 4
    p_core = me + 1 - 2 * core
    p_x = me + 2 - 4 * cx
    p_y = me + 4 - 8 * cy
    ka = ctx_ref.shape[1]
    km = act_ref.shape[1]

    def half_rows(c):
        base = 256 * c
        h1 = [
            base + 64 * (1 - cx) + 32 * (1 - cy),
            base + 64 * (1 - cx) + 32 * cy,
            base + 64 * cx + 32 * (1 - cy),
            base + 64 * cx + 32 * cy,
        ]
        base = base + 128
        h2 = [
            base + 64 * (1 - cy) + 32 * (1 - cx),
            base + 64 * (1 - cy) + 32 * cx,
            base + 64 * cy + 32 * (1 - cx),
            base + 64 * cy + 32 * cx,
        ]
        return h1 + h2

    rows = half_rows(1 - core) + half_rows(core)
    base1 = 256 * core + 64 * cx
    base2 = 256 * core + 128 + 64 * cy
    own1 = base1 + 32 * cy
    own2 = base2 + 32 * cx

    def w_copies(c, slot):
        cols = pl.ds(pl.multiple_of(c * W, W), W)
        out = []
        for j in range(ka // 1536):
            out.append(pltpu.make_async_copy(wo_ref.at[pl.ds(j * 1536, 1536), cols], w_v.at[slot, pl.ds(j * 1536, 1536)], w_sem.at[slot, len(out)]))
        for j in range(km // 1536):
            out.append(pltpu.make_async_copy(wd_ref.at[pl.ds(j * 1536, 1536), cols], w_v.at[slot, pl.ds(ka + j * 1536, 1536)], w_sem.at[slot, len(out)]))
        return out

    def x_copies(j):
        out = []
        for b, r in enumerate(rows):
            r = pl.multiple_of(r, 32)
            src = ctx_ref.at[pl.ds(r, 32), pl.ds(j * 1536, 1536)] if j * 1536 < ka else act_ref.at[pl.ds(r, 32), pl.ds(j * 1536 - ka, 1536)]
            out.append(pltpu.make_async_copy(src, x_v.at[pl.ds(32 * b, 32), pl.ds(j * 1536, 1536)], x_sem.at[j]))
        return out

    barrier = pltpu.get_barrier_semaphore()
    for p in (p_core, p_x, p_y):
        pl.semaphore_signal(barrier, inc=1, device_id={"tp": p}, device_id_type=MESH)
    n_slices = (ka + km) // 1536
    first = w_copies(0, 0)
    for j in range(n_slices):
        first[j].start()
        for cp in x_copies(j):
            cp.start()

    def remote(src, dst, k, c, to):
        return pltpu.make_async_remote_copy(
            src_ref=src, dst_ref=dst, send_sem=s_sem.at[k, lax.rem(c, SLOTS)], recv_sem=r_sem.at[k, c], device_id={"tp": to}, device_id_type=MESH
        )

    def y_at(r, n, c):
        return y_ref.at[pl.ds(pl.multiple_of(r, 32), n), pl.ds(pl.multiple_of(c * W, W), W)]

    def p0(c):
        return [remote(send0.at[lax.rem(c, 2)], recv0.at[c], 0, c, p_core)]

    def p1(c):
        s = lax.rem(c, SLOTS)
        return [remote(send1.at[s, 0], recv1.at[c, 0], 1, c, p_x), remote(send1.at[s, 1], recv1.at[c, 1], 2, c, p_y)]

    def p2(c):
        s = lax.rem(c, SLOTS)
        return [remote(send2.at[s, 0], recv2.at[c, 0], 3, c, p_y), remote(send2.at[s, 1], recv2.at[c, 1], 4, c, p_x)]

    def p3(c):
        return [remote(y_at(own1, 32, c), y_at(own1, 32, c), 5, c, p_y), remote(y_at(own2, 32, c), y_at(own2, 32, c), 6, c, p_x)]

    def p4(c):
        return [remote(y_at(base1, 64, c), y_at(base1, 64, c), 7, c, p_x), remote(y_at(base2, 64, c), y_at(base2, 64, c), 8, c, p_y)]

    def p5(c):
        half = 256 * core
        return [remote(y_at(half, 256, c), y_at(half, 256, c), 9, c, p_core)]

    def guard(cond, fn):
        if isinstance(cond, bool):
            if cond:
                fn()
        else:
            pl.when(cond)(fn)

    def drain(make, c):
        def fn():
            for d in make(c - SLOTS):
                d.wait_send()

        guard(c >= SLOTS, fn)

    def start(make, c):
        drain(make, c)
        for d in make(c):
            d.start()

    def stage0(c):
        for d in p0(c):
            d.wait_recv()
        k = lax.rem(c, SLOTS)
        drain(p1, c)
        for h in range(2):
            o = 128 * h
            send1[k, h] = (keep0[lax.rem(c, 2), o : o + 64] + recv0[c, o : o + 64].astype(F32)).astype(BF16)
            keep1[k, h] = keep0[lax.rem(c, 2), o + 64 : o + 128] + recv0[c, o + 64 : o + 128].astype(F32)
        for d in p1(c):
            d.start()

    def stage1(c):
        for d in p1(c):
            d.wait_recv()
        k = lax.rem(c, SLOTS)
        drain(p2, c)
        for h in range(2):
            send2[k, h] = (keep1[k, h, 0:32] + recv1[c, h, 0:32].astype(F32)).astype(BF16)
            keep2[k, h] = keep1[k, h, 32:64] + recv1[c, h, 32:64].astype(F32)
        for d in p2(c):
            d.start()

    def stage2(c):
        for d in p2(c):
            d.wait_recv()
        k = lax.rem(c, SLOTS)
        cols = pl.ds(pl.multiple_of(c * W, W), W)
        for h, r in enumerate((own1, own2)):
            y_ref[pl.ds(pl.multiple_of(r, 32), 32), cols] = (keep2[k, h] + recv2[c, h].astype(F32)).astype(BF16)
        start(p3, c)

    def stage3(c):
        for d in p3(c):
            d.wait_recv()
        start(p4, c)

    def stage4(c):
        for d in p4(c):
            d.wait_recv()
        start(p5, c)

    stages = (stage0, stage1, stage2, stage3, stage4)
    def serve(i):
        for k in ORDER:
            back = LAG[k]
            guard(i >= back, functools.partial(stages[k], i - back))

    def push_out(i, slot, theirs):
        send0[slot] = theirs.astype(BF16)
        for d in p0(i):
            d.start()

    total = None
    for j in range(n_slices):
        first[j].wait()
        pltpu.make_async_copy(ctx_ref.at[:, pl.ds(0, 1536)], x_v.at[:, pl.ds(j * 1536, 1536)], x_sem.at[j]).wait()
        if j == 0:
            for cp in w_copies(1, 1):
                cp.start()
        piece = jnp.dot(x_v[:, j * 1536 : (j + 1) * 1536], w_v[0, j * 1536 : (j + 1) * 1536], preferred_element_type=F32)
        total = piece if total is None else piece + total
    pl.semaphore_wait(barrier, 3)
    push_out(0, 0, total[0:256])
    keep0[0] = total[256:512]
    serve(0)

    def step(i, static):
        slot = i % 2 if static else lax.rem(i, 2)
        for cp in w_copies(i, slot):
            cp.wait()

        def ahead():
            for cp in w_copies(i + 1, 1 - slot):
                cp.start()

        guard(i + 1 < n_chunks, ahead)

        def sent():
            for d in p0(i - 2):
                d.wait_send()

        guard(i >= 2, sent)
        theirs = jnp.dot(x_v[0:256], w_v[slot], preferred_element_type=F32)
        early = jnp.dot(x_v[256:512, 0:EARLY], w_v[slot, 0:EARLY], preferred_element_type=F32)
        push_out(i, slot, theirs)
        keep0[slot] = jnp.dot(x_v[256:512, EARLY:], w_v[slot, EARLY:], preferred_element_type=F32) + early
        serve(i)

    for i in range(1, HEAD):
        step(i, True)

    def looped(i, carry):
        step(i, False)
        return carry

    lax.fori_loop(HEAD, n_chunks, looped, 0)
    for k, back in DRAIN:
        stages[k](n_chunks - back)
    for d in p0(n_chunks - 2) + p0(n_chunks - 1):
        d.wait_send()
    for c in range(n_chunks - SLOTS, n_chunks):
        for make in (p1, p2, p3, p4, p5):
            for d in make(c):
                d.wait_send()
    for c in range(n_chunks):
        for d in p5(c):
            d.wait_recv()


def store(y_ref, o_ref, sem):
    n = y_ref.shape[0] // STORES
    copies = [pltpu.make_async_copy(y_ref.at[pl.ds(j * n, n)], o_ref.at[pl.ds(j * n, n)], sem.at[j]) for j in range(STORES)]
    for cp in copies:
        cp.start()
    for cp in copies:
        cp.wait()


def solution(mesh):
    def device_step(ctx, w_out, act, w_down):
        rows, ka = ctx.shape
        km, cols = w_down.shape
        n = cols // W
        any_ = pl.BlockSpec(memory_space=pl.ANY)
        y = pl.pallas_call(
            functools.partial(kernel, n),
            out_shape=pltpu.VMEM((rows, cols), BF16),
            in_specs=[any_] * 4,
            out_specs=pl.BlockSpec(memory_space=pltpu.VMEM),
            scratch_shapes=[
                pltpu.VMEM((rows, ka + km), BF16),
                pltpu.VMEM((2, ka + km, W), BF16),
                pltpu.VMEM((n, 256, W), BF16),
                pltpu.VMEM((n, 2, 64, W), BF16),
                pltpu.VMEM((n, 2, 32, W), BF16),
                pltpu.VMEM((2, 256, W), BF16),
                pltpu.VMEM((SLOTS, 2, 64, W), BF16),
                pltpu.VMEM((SLOTS, 2, 32, W), BF16),
                pltpu.VMEM((2, 256, W), F32),
                pltpu.VMEM((SLOTS, 2, 64, W), F32),
                pltpu.VMEM((SLOTS, 2, 32, W), F32),
                pltpu.SemaphoreType.DMA(((ka + km) // 1536,)),
                pltpu.SemaphoreType.DMA((2, (ka + km) // 1536)),
                pltpu.SemaphoreType.DMA((10, SLOTS)),
                pltpu.SemaphoreType.DMA((10, n)),
            ],
            compiler_params=pltpu.CompilerParams(collective_id=0, has_side_effects=True, vmem_limit_bytes=VMEM_LIMIT),
            cost_estimate=pl.CostEstimate(flops=2 * rows * (ka + km) * cols, bytes_accessed=2 * (ka + km) * cols, transcendentals=0),
        )(ctx, w_out, act, w_down)
        return pl.pallas_call(
            store,
            out_shape=jax.ShapeDtypeStruct((rows, cols), BF16),
            in_specs=[pl.BlockSpec(memory_space=pltpu.VMEM)],
            out_specs=pl.BlockSpec(memory_space=pl.ANY),
            scratch_shapes=[pltpu.SemaphoreType.DMA((STORES,))],
            compiler_params=pltpu.CompilerParams(vmem_limit_bytes=1024 * 1024),
            cost_estimate=pl.CostEstimate(flops=0, bytes_accessed=2 * rows * cols, transcendentals=0),
        )(y)

    return jax.shard_map(
        device_step,
        mesh=mesh,
        in_specs=(P("data", "tp"), P("tp", None), P("data", "tp"), P("tp", None)),
        out_specs=P("data", None),
        check_vma=False,
    )
```
